32 devices in a mesh: row: 4 (over y, x), col: 8 (over z, core).
Axes of the slice: x: 2, y: 2, z: 4, core: 2. Of those that a mesh axis runs over, the one named last changes fastest.
Arguments:
- view_a: bfloat16 [3072, 8192], P(('row', 'col')), may hold values from -1000 to 1000
- view_b: bfloat16 [3072, 8192], P(('row', 'col')), may hold values from -1000 to 1000
Outputs:
- correlation: float32 [8192, 8192], P('row', 'col')
- loss: float32 [], replicated
The draws below stay inside these ranges and needn't reach their ends.
All inputs are finite; a program needn't handle non-finite values.
Results may differ from the reference program's by a relative error of at most 0.0013.
Values may be sent and summed in bfloat16 or wider, within the bound.
A program may use at most 192 MiB of HBM per device.

```python
import jax
import jax.numpy as jnp
from jax import lax

D = 8192
TOKENS = 3072


def draw_pair(key):
    keys = jax.random.split(jax.random.fold_in(key, 11), 6)
    ramp = jnp.arange(TOKENS, dtype=jnp.float32) / max(TOKENS - 1, 1)
    row_scale = (1.0 + 2.0 * ramp) * jnp.exp(jax.random.uniform(keys[0], (TOKENS,), jnp.float32, 0.0, jnp.log(3.0)))
    col_scale = jnp.exp(jax.random.uniform(keys[1], (D,), jnp.float32, 0.0, jnp.log(10.0)))
    mixing = jax.random.uniform(keys[2], (D,), jnp.float32, 0.2, 0.95)
    offset = 0.5 * jax.random.normal(keys[3], (D,), jnp.float32)
    base = jax.random.normal(keys[4], (TOKENS, D), jnp.float32)
    noise = jax.random.normal(keys[5], (TOKENS, D), jnp.float32)
    other = mixing * base + jnp.sqrt(1.0 - mixing * mixing) * noise
    scale = row_scale[:, None] * col_scale[None, :]
    first = jnp.clip((base + offset) * scale, -1000.0, 1000.0)
    second = jnp.clip((other + offset) * scale, -1000.0, 1000.0)
    return (first, second)


def draw_view_a(key, part):
    return draw_pair(key)[0].astype(jnp.bfloat16)


def draw_view_b(key, part):
    return draw_pair(key)[1].astype(jnp.bfloat16)


def setup_inputs(seed: int = 0) -> dict:
    seeds = jax.random.split(jax.random.key(seed), 3)
    return {
        "view_a": draw_view_a(jax.random.fold_in(seeds[2], 71), 0),
        "view_b": draw_view_b(jax.random.fold_in(seeds[2], 71), 0),
    }


def normalize(view):
    values = view.astype(jnp.float32)
    count = view.shape[0]
    mean = lax.optimization_barrier(jnp.sum(values, 0)) / count
    var = lax.optimization_barrier(jnp.sum(values * values, 0)) / count - mean * mean
    return ((values - mean) * lax.rsqrt(var + 1e-05)).astype(jnp.bfloat16)

def reference(view_a, view_b):
    norm_a = normalize(view_a).astype(jnp.float32)
    norm_b = normalize(view_b).astype(jnp.float32)
    product = lax.dot_general(norm_a, norm_b, (((0,), (0,)), ((), ())), precision=lax.Precision.HIGHEST, preferred_element_type=jnp.float32)
    correlation = product / view_a.shape[0]
    diag = jnp.diagonal(correlation)
    total = 0.0051 * jnp.sum(correlation * correlation) + jnp.sum((1.0 - diag) ** 2 - 0.0051 * diag * diag)
    loss = total / view_a.shape[1]
    return (correlation, loss)
```

```python
import functools

import jax
import jax.numpy as jnp
from jax import lax
from jax.experimental import pallas as pl
from jax.experimental.pallas import tpu as pltpu
from jax.sharding import PartitionSpec as P

MESH = pl.DeviceIdType.MESH
F32 = jnp.float32
BF16 = jnp.bfloat16


def body(
    n_row, n_col, width,
    a_in, b_in, out, loss_out,
    a_all, b_all, nb, stat_a, stat_b, coef_a, coef_b, shares,
    s_a, r_a, s_b, r_b, s_sa, r_sa, s_sb, r_sb, s_line, r_line, s_fwd, r_fwd,
    s_loss, r_loss, own_sem,
):
    t = a_in.shape[0]
    rb = a_in.shape[1] // n_row
    cb = b_in.shape[1] // n_col
    count = t * n_row * n_col
    n_z = n_col // 2
    r = lax.axis_index("row")
    c = lax.axis_index("col")
    z = c // 2
    k = c % 2
    mine = pl.ds(pl.multiple_of(r * t, t), t)

    def row_mate(i):
        return (r + i) % n_row

    def col_mate(j):
        return (c + j) % n_col

    def remote(src, dst, ss, rs, dev):
        return pltpu.make_async_remote_copy(
            src_ref=src, dst_ref=dst, send_sem=ss, recv_sem=rs, device_id=dev, device_id_type=MESH
        )

    own_a = pltpu.make_async_copy(
        a_in.at[:, pl.ds(pl.multiple_of(r * rb, rb), rb)], a_all.at[c, mine], own_sem.at[0]
    )
    own_b = pltpu.make_async_copy(
        b_in.at[:, pl.ds(pl.multiple_of(c * cb, cb), cb)], b_all.at[c, mine], own_sem.at[1]
    )
    own_a.start()
    own_b.start()

    barrier = pltpu.get_barrier_semaphore()

    def greet(i, carry):
        dst = (r * n_col + c + i) % (n_row * n_col)
        pl.semaphore_signal(barrier, inc=1, device_id=(dst // n_col, dst % n_col), device_id_type=MESH)
        return carry

    lax.fori_loop(1, n_row * n_col, greet, 0)
    pl.semaphore_wait(barrier, n_row * n_col - 1)

    def send_a(i):
        dst = row_mate(i)
        cols = pl.ds(pl.multiple_of(dst * rb, rb), rb)
        return remote(a_in.at[:, cols], a_all.at[c, mine], s_a.at[i], r_a.at[i], (dst, c))

    def got_a(i):
        src = row_mate(n_row - i)
        rows = pl.ds(pl.multiple_of(src * t, t), t)
        return remote(a_all.at[c, rows], a_all.at[c, rows], s_a.at[i], r_a.at[i], (src, c))

    def send_b(j):
        dst = col_mate(j)
        cols = pl.ds(pl.multiple_of(dst * cb, cb), cb)
        return remote(b_in.at[:, cols], b_all.at[c, mine], s_b.at[j], r_b.at[j], (r, dst))

    def got_b(j):
        src = col_mate(n_col - j)
        return remote(b_all.at[src, mine], b_all.at[src, mine], s_b.at[j], r_b.at[j], (r, src))

    for i in range(1, n_row):
        send_a(i).start()

    def line(way, chunk, p, dev_c):
        rows = pl.ds(pl.multiple_of(p * t, t), t)
        ref = a_all.at[chunk, rows]
        return remote(ref, ref, s_line.at[way, chunk, p], r_line.at[chunk, p], (r, dev_c))

    partner = z * 2 + (1 - k)

    def up(chunk, p):
        return line(0, chunk, p, lax.min(c + 2, n_col - 2 + k))

    def down(chunk, p):
        return line(1, chunk, p, lax.max(c - 2, k))

    def across(chunk, p):
        return line(2, chunk, p, partner)

    can_up = z < n_z - 1
    can_down = z > 0

    def slice_at(o):
        return (r + n_row - o) % n_row

    def send_line(o):
        p = slice_at(o)

        @pl.when(can_up)
        def _():
            up(c, p).start()

        @pl.when(can_down)
        def _():
            down(c, p).start()

        across(c, p).start()

    own_a.wait()
    send_line(0)

    for dist in range(n_z - 1, 0, -1):
        for side in range(2):
            zz = z - dist if side == 0 else z + dist

            @pl.when(jnp.logical_and(zz >= 0, zz < n_z))
            def _():
                for other in range(2):
                    send_b((zz * 2 + (k + other) % 2 + n_col - c) % n_col).start()

    send_b((partner + n_col - c) % n_col).start()

    for o in range(1, n_row):
        got_a(o).wait_recv()
        if o < n_row - 1:
            send_line(o)

    def moments_a(q, carry):
        cols = pl.ds(pl.multiple_of(q * 128, 128), 128)
        x = a_all[c, :, cols].astype(F32)
        stat_a[c, 0:1, cols] = jnp.sum(x, 0, keepdims=True)
        stat_a[c, 1:2, cols] = jnp.sum(x * x, 0, keepdims=True)
        return carry

    lax.fori_loop(0, rb // 128, moments_a, 0)

    def send_sa(j):
        return remote(stat_a.at[c], stat_a.at[c], s_sa.at[j], r_sa.at[j], (r, col_mate(j)))

    def got_sa(j):
        src = col_mate(n_col - j)
        return remote(stat_a.at[src], stat_a.at[src], s_sa.at[j], r_sa.at[j], (r, src))

    for j in range(1, n_col):
        send_sa(j).start()
    if n_row > 1:
        send_line(n_row - 1)

    def send_fwd(i, g):
        return remote(b_all.at[g, mine], b_all.at[g, mine], s_fwd.at[i, g], r_fwd.at[i, g], (row_mate(i), c))

    def got_fwd(i, g):
        src = row_mate(n_row - i)
        rows = pl.ds(pl.multiple_of(src * t, t), t)
        return remote(b_all.at[g, rows], b_all.at[g, rows], s_fwd.at[i, g], r_fwd.at[i, g], (src, c))

    def each_chunk(d, do):
        for side in range(2):
            zz = z - d if side == 0 else z + d
            ok = (zz >= 0) if side == 0 else jnp.logical_and(zz < n_z, d > 0)

            @pl.when(ok)
            def _():
                do(zz * 2 + k, side)
                do(zz * 2 + (1 - k), side)

    def forward(d, carry):
        def do(g, side):
            for i in range(1, n_row):
                send_fwd(i, g).start()

        each_chunk(d, do)
        return carry

    own_b.wait()
    near = 1 + (n_col - 2) * (1 - k)
    got_b(near).wait_recv()
    forward(0, 0)
    for j in range(1, n_col):
        @pl.when(j != near)
        def _():
            got_b(j).wait_recv()


    def moments_b(q, carry):
        cols = pl.ds(pl.multiple_of(q * 128, 128), 128)
        total = jnp.zeros((1, 128), F32)
        squares = jnp.zeros((1, 128), F32)
        for g in range(n_col):
            x = b_all[g, mine, cols].astype(F32)
            total = total + jnp.sum(x, 0, keepdims=True)
            squares = squares + jnp.sum(x * x, 0, keepdims=True)
        stat_b[r, 0:1, cols] = total
        stat_b[r, 1:2, cols] = squares
        return carry

    lax.fori_loop(0, cb // 128, moments_b, 0)

    def send_sb(i):
        return remote(stat_b.at[r], stat_b.at[r], s_sb.at[i], r_sb.at[i], (row_mate(i), c))

    def got_sb(i):
        src = row_mate(n_row - i)
        return remote(stat_b.at[src], stat_b.at[src], s_sb.at[i], r_sb.at[i], (src, c))

    for i in range(1, n_row):
        send_sb(i).start()

    lax.fori_loop(1, n_z, forward, 0)

    def clear(q, carry):
        rows = pl.ds(pl.multiple_of(q * 64, 64), 64)
        out[rows, :] = jnp.zeros((64, cb), F32)
        return carry

    lax.fori_loop(0, rb // 64, clear, 0)

    for j in range(1, n_col):
        got_sa(j).wait_recv()
    for i in range(1, n_row):
        got_sb(i).wait_recv()

    def coefs(stat, coef):
        sums = jnp.sum(stat[...], 0)
        mean = sums[0:1] / count
        var = sums[1:2] / count - mean * mean
        coef[0:1, :] = mean
        coef[1:2, :] = lax.rsqrt(var + 1e-05)

    coefs(stat_a, coef_a)
    coefs(stat_b, coef_b)

    tile = min(1024, rb)

    def wait_fwd(zz):
        for g in range(2):
            for i in range(1, n_row):
                got_fwd(i, zz * 2 + g).wait_recv()

    def process(zz):
        for p in range(n_row):
            across(zz * 2 + (1 - k), p).wait_recv()
        wait_fwd(zz)
        multiply(zz, pl.ds(0, n_row * t), n_row * t)

    def multiply(zz, rows, height):
        pair = pl.ds(zz * 2, 2)
        depth = 2 * height

        def norm_b(q, carry):
            cols = pl.ds(pl.multiple_of(q * 128, 128), 128)
            x = b_all[pair, rows, cols].astype(F32).reshape(depth, 128)
            nb[0:depth, cols] = ((x - coef_b[0:1, cols]) * coef_b[1:2, cols]).astype(BF16)
            return carry

        lax.fori_loop(0, cb // 128, norm_b, 0)

        def mul(q, carry):
            cols = pl.ds(pl.multiple_of(q * tile, tile), tile)
            x = a_all[pair, rows, cols].astype(F32).reshape(depth, tile)
            na = ((x - coef_a[0:1, cols]) * coef_a[1:2, cols]).astype(BF16)
            out[cols, :] += lax.dot_general(
                na, nb[0:depth, :], (((0,), (0,)), ((), ())), preferred_element_type=F32
            )
            return carry

        lax.fori_loop(0, rb // tile, mul, 0)

    def process_all(d):
        def one(side, carry):
            zz = jnp.where(side == 0, z - d, z + d)
            ok = jnp.logical_and(zz >= 0, zz < n_z)
            ok = jnp.logical_and(ok, jnp.logical_or(side == 0, d > 0))

            @pl.when(ok)
            def _():
                process(zz)

            return carry

        lax.fori_loop(0, 2, one, 0)

    def relay(d):
        from_low = z - d >= 0
        from_high = z + d < n_z
        low = (z - d) * 2 + k
        high = (z + d) * 2 + k
        for o in range(n_row):
            p = slice_at(o)

            @pl.when(from_low)
            def _():
                up(low, p).wait_recv()

                @pl.when(can_up)
                def _():
                    up(low, p).start()

                across(low, p).start()

            @pl.when(from_high)
            def _():
                down(high, p).wait_recv()

                @pl.when(can_down)
                def _():
                    down(high, p).start()

                across(high, p).start()

    def last():
        zz = jnp.where(z == 0, n_z - 1, 0)
        g = zz * 2 + k

        @pl.when(jnp.logical_or(z == 0, z == n_z - 1))
        def _():
            wait_fwd(zz)

            def one(o, carry):
                p = slice_at(o)
                up(g, p).wait_recv()
                across(g, p).start()
                across(zz * 2 + (1 - k), p).wait_recv()
                multiply(zz, pl.ds(pl.multiple_of(p * t, t), t), t)
                return carry

            lax.fori_loop(0, n_row, one, 0)

    def step(d, carry):
        @pl.when(d + 1 < n_z - 1)
        def _():
            relay(d + 1)

        process_all(d)

        return carry

    lax.fori_loop(0, max(n_z - 1, 1), step, 0)
    if n_z > 1:
        last()

    def part(q, carry):
        rows = pl.ds(pl.multiple_of(q * 8, 8), 8)
        x = out[rows, :] * (1.0 / count)
        out[rows, :] = x
        row_ids = r * rb + q * 8 + lax.broadcasted_iota(jnp.int32, (8, cb), 0)
        col_ids = c * cb + lax.broadcasted_iota(jnp.int32, (8, cb), 1)
        sq = x * x
        return carry + jnp.where(row_ids == col_ids, (1.0 - x) * (1.0 - x), 0.0051 * sq)

    share = lax.fori_loop(0, rb // 8, part, jnp.zeros((8, cb), F32), unroll=4)
    folded = share[:, 0:128]
    for q in range(1, cb // 128):
        folded = folded + share[:, q * 128 : (q + 1) * 128]
    n_dev = n_row * n_col
    me = r * n_col + c
    shares[me] = jnp.sum(folded, 0, keepdims=True)

    def send_share(i):
        dst = (me + i) % n_dev
        ref = shares.at[me]
        return remote(ref, ref, s_loss.at[i], r_loss.at[i], (dst // n_col, dst % n_col))

    def got_share(i):
        src = (me + n_dev - i) % n_dev
        ref = shares.at[src]
        return remote(ref, ref, s_loss.at[i], r_loss.at[i], (src // n_col, src % n_col))

    def each_peer(do):
        def one(i, carry):
            do(i)
            return carry

        lax.fori_loop(1, n_dev, one, 0)

    each_peer(lambda i: send_share(i).start())

    for i in range(1, n_row):
        send_a(i).wait_send()
        send_sb(i).wait_send()
    for j in range(1, n_col):
        send_b(j).wait_send()
        send_sa(j).wait_send()

    def drain(g, carry):
        for i in range(1, n_row):
            send_fwd(i, g).wait_send()
        zz = g // 2
        for p in range(n_row):
            @pl.when(g % 2 == k)
            def _():
                @pl.when(jnp.logical_and(zz <= z, can_up))
                def _():
                    up(g, p).wait_send()

                @pl.when(jnp.logical_and(zz >= z, can_down))
                def _():
                    down(g, p).wait_send()

                across(g, p).wait_send()

        return carry

    lax.fori_loop(0, n_col, drain, 0)

    each_peer(lambda i: got_share(i).wait_recv())
    loss_out[...] = jnp.broadcast_to(
        jnp.sum(jnp.sum(shares[...], 0), keepdims=True) / width, loss_out.shape
    )
    each_peer(lambda i: send_share(i).wait_send())


def hbm(x):
    return pltpu.with_memory_space_constraint(x, pltpu.HBM)


def emit_body(pieces, x, out, sem):
    height = x.shape[0] // pieces

    def move(i):
        rows = pl.ds(i * height, height)
        return pltpu.make_async_copy(x.at[rows], out.at[rows], sem.at[i])

    for i in range(pieces):
        move(i).start()
    for i in range(pieces):
        move(i).wait()


def emit(x):
    return pl.pallas_call(
        functools.partial(emit_body, 8),
        out_shape=jax.ShapeDtypeStruct(x.shape, x.dtype),
        in_specs=[pl.BlockSpec(memory_space=pltpu.VMEM)],
        out_specs=pl.BlockSpec(memory_space=pltpu.HBM),
        scratch_shapes=[pltpu.SemaphoreType.DMA((8,))],
        compiler_params=pltpu.CompilerParams(vmem_limit_bytes=16 << 20),
        name="emit",
    )(x)


def shards(view_a, view_b):
    t, width = view_a.shape
    n_row = lax.axis_size("row")
    n_col = lax.axis_size("col")
    rb = width // n_row
    cb = width // n_col
    count = t * n_row * n_col
    n_chunk = t * n_row
    dma = pltpu.SemaphoreType.DMA
    size = 2 * (count * (rb + cb) + 2 * n_chunk * cb + 2 * t * width) + 4 * rb * cb
    product, loss = pl.pallas_call(
        functools.partial(body, n_row, n_col, width),
        out_shape=(
            jax.ShapeDtypeStruct((rb, cb), F32),
            jax.ShapeDtypeStruct((8, 128), F32),
        ),
        in_specs=[pl.BlockSpec(memory_space=pltpu.HBM)] * 2,
        out_specs=(pl.BlockSpec(memory_space=pltpu.VMEM),) * 2,
        scratch_shapes=[
            pltpu.VMEM((n_col, n_chunk, rb), BF16),
            pltpu.VMEM((n_col, n_chunk, cb), BF16),
            pltpu.VMEM((2 * n_chunk, cb), BF16),
            pltpu.VMEM((n_col, 2, rb), F32),
            pltpu.VMEM((n_row, 2, cb), F32),
            pltpu.VMEM((2, rb), F32),
            pltpu.VMEM((2, cb), F32),
            pltpu.VMEM((n_row * n_col, 1, 128), F32),
            dma((n_row,)), dma((n_row,)),
            dma((n_col,)), dma((n_col,)),
            dma((n_col,)), dma((n_col,)),
            dma((n_row,)), dma((n_row,)),
            dma((3, n_col, n_row)), dma((n_col, n_row)),
            dma((n_row, n_col)), dma((n_row, n_col)),
            dma((n_row * n_col,)), dma((n_row * n_col,)),
            dma((2,)),
        ],
        compiler_params=pltpu.CompilerParams(
            collective_id=0, has_side_effects=True, vmem_limit_bytes=min(size + (12 << 20), 60 << 20)
        ),
        name="twins",
    )(hbm(view_a), hbm(view_b))
    return emit(product), loss[0, 0]


def solution(mesh):
    return jax.shard_map(
        shards,
        mesh=mesh,
        in_specs=(P(("row", "col"), None), P(("row", "col"), None)),
        out_specs=(P("row", "col"), P()),
        check_vma=False,
    )
```

```python
import functools

import jax
import jax.numpy as jnp
from jax import lax
from jax.experimental import pallas as pl
from jax.experimental.pallas import tpu as pltpu
from jax.sharding import PartitionSpec as P

MESH = pl.DeviceIdType.MESH
F32 = jnp.float32
BF16 = jnp.bfloat16
TAIL = 4


def body(
    n_row, n_col, width,
    a_in, b_in, out, loss_out,
    a_all, b_all, nb, stat_a, stat_b, coef_a, coef_b, partial, shares,
    r_a, r_b, s_line, r_line, r_across, s_tail, r_tail, x_tail, r_fwd, once,
):
    t = a_in.shape[0]
    rb = a_in.shape[1] // n_row
    cb = b_in.shape[1] // n_col
    count = t * n_row * n_col
    n_z = n_col // 2
    r = lax.axis_index("row")
    c = lax.axis_index("col")
    z = c // 2
    k = c % 2
    mine = pl.ds(pl.multiple_of(r * t, t), t)

    def row_mate(i):
        return (r + i) % n_row

    def col_mate(j):
        return (c + j) % n_col

    def remote(src, dst, ss, rs, dev):
        return pltpu.make_async_remote_copy(
            src_ref=src, dst_ref=dst, send_sem=ss, recv_sem=rs, device_id=dev, device_id_type=MESH
        )

    own_a = pltpu.make_async_copy(
        a_in.at[:, pl.ds(pl.multiple_of(r * rb, rb), rb)], a_all.at[c, mine], once.at[0]
    )
    own_b = pltpu.make_async_copy(
        b_in.at[:, pl.ds(pl.multiple_of(c * cb, cb), cb)], b_all.at[c, mine], once.at[1]
    )
    own_a.start()
    own_b.start()

    barrier = pltpu.get_barrier_semaphore()

    def greet(i, carry):
        dst = (r * n_col + c + i) % (n_row * n_col)
        pl.semaphore_signal(barrier, inc=1, device_id=(dst // n_col, dst % n_col), device_id_type=MESH)
        return carry

    lax.fori_loop(1, n_row * n_col, greet, 0)
    pl.semaphore_wait(barrier, n_row * n_col - 1)

    def sent(ref, sem):
        remote(ref, ref, sem, sem, (r, c)).wait_send()

    def landed(ref, sem):
        remote(ref, ref, sem, sem, (r, c)).wait_recv()

    def send_a(i):
        dst = row_mate(i)
        cols = pl.ds(pl.multiple_of(dst * rb, rb), rb)
        return remote(a_in.at[:, cols], a_all.at[c, mine], once.at[2], r_a.at[i], (dst, c))

    def got_a(i):
        src = row_mate(n_row - i)
        rows = pl.ds(pl.multiple_of(src * t, t), t)
        return remote(a_all.at[c, rows], a_all.at[c, rows], once.at[2], r_a.at[i], (src, c))

    def send_b(j):
        dst = col_mate(j)
        cols = pl.ds(pl.multiple_of(dst * cb, cb), cb)
        return remote(b_in.at[:, cols], b_all.at[c, mine], once.at[3], r_b.at[z], (r, dst))

    for i in range(1, n_row):
        send_a(i).start()

    def block(chunk, p):
        return a_all.at[chunk, pl.ds(pl.multiple_of(p * t, t), t)]

    partner = z * 2 + (1 - k)
    above = (r, lax.min(c + 2, n_col - 2 + k))
    below = (r, lax.max(c - 2, k))
    beside = (r, partner)

    def up(chunk, p):
        ref = block(chunk, p)
        return remote(ref, ref, s_line.at[0, chunk // 2], r_line.at[chunk // 2, p], above)

    def down(chunk, p):
        ref = block(chunk, p)
        return remote(ref, ref, s_line.at[1, chunk // 2], r_line.at[chunk // 2, p], below)

    def across(chunk, p):
        ref = block(chunk, p)
        far = lax.max(chunk // 2 - z, z - chunk // 2) == n_z - 1
        slot = jnp.where(far, n_z + p, chunk // 2)
        return remote(ref, ref, once.at[4], r_across.at[slot], beside)

    wide = rb // TAIL

    def slab(chunk, p, f):
        return a_all.at[
            chunk, pl.ds(pl.multiple_of(p * t, t), t), pl.ds(pl.multiple_of(f * wide, wide), wide)
        ]

    def tail(way, chunk, p, f):
        ref = slab(chunk, p, f)
        return remote(ref, ref, s_tail.at[way], r_tail.at[f], above if way == 0 else below)

    def tail_across(chunk, p, f):
        ref = slab(chunk, p, f)
        return remote(ref, ref, once.at[4], x_tail.at[f], beside)

    can_up = z < n_z - 1
    can_down = z > 0

    def slice_at(o):
        return (r + n_row - o) % n_row

    def send_line(o):
        p = slice_at(o)

        @pl.when(can_up)
        def _():
            up(c, p).start()

        @pl.when(can_down)
        def _():
            down(c, p).start()

        across(c, p).start()

    own_a.wait()
    send_line(0)

    for dist in range(n_z - 1, 0, -1):
        for side in range(2):
            zz = z - dist if side == 0 else z + dist

            @pl.when(jnp.logical_and(zz >= 0, zz < n_z))
            def _():
                for other in range(2):
                    send_b((zz * 2 + (k + other) % 2 + n_col - c) % n_col).start()

    send_b((partner + n_col - c) % n_col).start()

    for o in range(1, n_row):
        got_a(o).wait_recv()
        if o < n_row - 1:
            send_line(o)

    def moments_a(q, carry):
        cols = pl.ds(pl.multiple_of(q * 128, 128), 128)
        x = a_all[c, :, cols].astype(F32)
        stat_a[c, 0:1, cols] = jnp.sum(x, 0, keepdims=True)
        stat_a[c, 1:2, cols] = jnp.sum(x * x, 0, keepdims=True)
        return carry

    lax.fori_loop(0, rb // 128, moments_a, 0)

    def send_sa(j):
        return remote(stat_a.at[c], stat_a.at[c], once.at[5], once.at[6], (r, col_mate(j)))

    for j in range(1, n_col):
        send_sa(j).start()
    if n_row > 1:
        send_line(n_row - 1)

    def send_fwd(i, g):
        return remote(b_all.at[g, mine], b_all.at[g, mine], once.at[7], r_fwd.at[g // 2], (row_mate(i), c))

    def each_chunk(d, do):
        for side in range(2):
            zz = z - d if side == 0 else z + d
            ok = (zz >= 0) if side == 0 else jnp.logical_and(zz < n_z, d > 0)

            @pl.when(ok)
            def _():
                do(zz * 2 + k, side)
                do(zz * 2 + (1 - k), side)

    def forward(d, carry):
        def do(g, side):
            for i in range(1, n_row):
                send_fwd(i, g).start()

        each_chunk(d, do)
        return carry

    def relay(d, o):
        split = isinstance(d, int) and d == n_z - 2 and o == n_row - 1
        from_low = z - d >= 0
        from_high = z + d < n_z
        low = (z - d) * 2 + k
        high = (z + d) * 2 + k
        p = slice_at(o)

        @pl.when(from_low)
        def _():
            up(low, p).wait_recv()

            @pl.when(can_up)
            def _():
                if split:
                    for f in range(TAIL):
                        tail(0, low, p, f).start()
                else:
                    up(low, p).start()

            across(low, p).start()

        @pl.when(from_high)
        def _():
            down(high, p).wait_recv()

            @pl.when(can_down)
            def _():
                if split:
                    for f in range(TAIL):
                        tail(1, high, p, f).start()
                else:
                    down(high, p).start()

            across(high, p).start()

    def arrive(d):
        for side in range(2):
            zz = z - d if side == 0 else z + d

            @pl.when(jnp.logical_and(zz >= 0, zz < n_z))
            def _():
                landed(b_all.at[pl.ds(zz * 2, 2), mine], r_b.at[zz])

    own_b.wait()
    landed(b_all.at[partner, mine], r_b.at[z])
    forward(0, 0)
    early = n_z > 2
    for o in range(n_row if early else 0):
        relay(1, o)
        if o + 1 < min(n_row, n_z):
            arrive(o + 1)
            forward(o + 1, 0)

    def rest(d, carry):
        arrive(d)
        forward(d, 0)
        return carry

    lax.fori_loop(min(n_row, n_z) if early else 1, n_z, rest, 0)

    for o in range(n_row if n_z > 3 else 0):
        relay(2, o)

    def moments_b(q, carry):
        cols = pl.ds(pl.multiple_of(q * 128, 128), 128)
        total = jnp.zeros((1, 128), F32)
        squares = jnp.zeros((1, 128), F32)
        for g in range(n_col):
            x = b_all[g, mine, cols].astype(F32)
            total = total + jnp.sum(x, 0, keepdims=True)
            squares = squares + jnp.sum(x * x, 0, keepdims=True)
        stat_b[r, 0:1, cols] = total
        stat_b[r, 1:2, cols] = squares
        return carry

    lax.fori_loop(0, cb // 128, moments_b, 0)

    def send_sb(i):
        return remote(stat_b.at[r], stat_b.at[r], once.at[8], once.at[9], (row_mate(i), c))

    for i in range(1, n_row):
        send_sb(i).start()

    def clear(q, carry):
        rows = pl.ds(pl.multiple_of(q * 64, 64), 64)
        out[rows, :] = jnp.zeros((64, cb), F32)
        return carry

    lax.fori_loop(0, rb // 64, clear, 0)

    landed(stat_a.at[pl.ds(0, n_col - 1)], once.at[6])
    landed(stat_b.at[pl.ds(0, n_row - 1)], once.at[9])

    def coefs(stat, coef):
        sums = jnp.sum(stat[...], 0)
        mean = sums[0:1] / count
        var = sums[1:2] / count - mean * mean
        coef[0:1, :] = mean
        coef[1:2, :] = lax.rsqrt(var + 1e-05)

    coefs(stat_a, coef_a)
    coefs(stat_b, coef_b)

    tile = min(1024, rb)

    def wait_fwd(zz):
        landed(b_all.at[pl.ds(zz * 2, 2), pl.ds(0, (n_row - 1) * t)], r_fwd.at[zz])

    def process(zz):
        landed(a_all.at[zz * 2 + (1 - k)], r_across.at[zz])
        wait_fwd(zz)
        multiply(zz, pl.ds(0, n_row * t), n_row * t)

    def normalize_b(zz, rows, height):
        def one(q, carry):
            cols = pl.ds(pl.multiple_of(q * 128, 128), 128)
            x = b_all[pl.ds(zz * 2, 2), rows, cols].astype(F32).reshape(2 * height, 128)
            nb[0 : 2 * height, cols] = ((x - coef_b[0:1, cols]) * coef_b[1:2, cols]).astype(BF16)
            return carry

        lax.fori_loop(0, cb // 128, one, 0)

    def product(zz, rows, height, cols, width):
        x = a_all[pl.ds(zz * 2, 2), rows, cols].astype(F32).reshape(2 * height, width)
        na = ((x - coef_a[0:1, cols]) * coef_a[1:2, cols]).astype(BF16)
        return lax.dot_general(
            na, nb[0 : 2 * height, :], (((0,), (0,)), ((), ())), preferred_element_type=F32
        )

    def multiply(zz, rows, height):
        normalize_b(zz, rows, height)

        def mul(q, carry):
            cols = pl.ds(pl.multiple_of(q * tile, tile), tile)
            out[cols, :] += product(zz, rows, height, cols, tile)
            return carry

        lax.fori_loop(0, rb // tile, mul, 0)

    def process_all(d):
        def one(side, carry):
            zz = jnp.where(side == 0, z - d, z + d)
            ok = jnp.logical_and(zz >= 0, zz < n_z)
            ok = jnp.logical_and(ok, jnp.logical_or(side == 0, d > 0))

            @pl.when(ok)
            def _():
                process(zz)

            return carry

        lax.fori_loop(0, 2, one, 0)

    at_end = jnp.logical_and(n_z > 2, jnp.logical_or(z == 0, z == n_z - 1))

    def finish(x):
        x = x * (1.0 / count)
        partial[...] += jnp.sum((x * x).reshape(x.shape[0] // 8, 8, cb), 0)
        return x

    def last():
        zz = jnp.where(z == 0, n_z - 1, 0)
        g = zz * 2 + k
        other = zz * 2 + (1 - k)

        @pl.when(jnp.logical_or(z == 0, z == n_z - 1))
        def _():
            wait_fwd(zz)

            def one(o, carry):
                p = slice_at(o)
                up(g, p).wait_recv()
                across(g, p).start()
                landed(block(other, p), r_across.at[n_z + p])
                multiply(zz, pl.ds(pl.multiple_of(p * t, t), t), t)
                return carry

            lax.fori_loop(0, n_row - 1 if n_z > 2 else n_row, one, 0)
            if n_z > 2:
                p = slice_at(n_row - 1)
                rows = pl.ds(pl.multiple_of(p * t, t), t)
                normalize_b(zz, rows, t)

                def some(f, carry):
                    landed(slab(g, p, f), r_tail.at[f])
                    tail_across(g, p, f).start()
                    landed(slab(other, p, f), x_tail.at[f])
                    cols = pl.ds(pl.multiple_of(f * wide, wide), wide)
                    out[cols, :] = finish(out[cols, :] + product(zz, rows, t, cols, wide))
                    return carry

                lax.fori_loop(0, TAIL, some, 0)

    def step(d, carry):
        process_all(d)

        if n_z > 5:
            @pl.when(d + 3 < n_z - 2)
            def _():
                for o in range(n_row):
                    relay(d + 3, o)

        if n_z > 4:
            @pl.when(d + 3 == n_z - 2)
            def _():
                for o in range(n_row):
                    relay(n_z - 2, o)

        return carry

    lax.fori_loop(0, max(n_z - 1, 1), step, 0)
    partial[...] = jnp.zeros((8, cb), F32)
    if n_z > 1:
        last()

    @pl.when(jnp.logical_not(at_end))
    def _():
        def part(q, carry):
            rows = pl.ds(pl.multiple_of(q * 64, 64), 64)
            out[rows, :] = finish(out[rows, :])
            return carry

        lax.fori_loop(0, rb // 64, part, 0)

    folded = partial[:, 0:128]
    for q in range(1, cb // 128):
        folded = folded + partial[:, q * 128 : (q + 1) * 128]
    folded = jnp.sum(0.0051 * folded, 0, keepdims=True)

    def diagonal(q, carry):
        first = c * cb + q * 128 - r * rb
        inside = jnp.logical_and(first >= 0, first < rb)
        rows = pl.ds(pl.multiple_of(jnp.where(inside, first, 0), 128), 128)
        x = out[rows, pl.ds(pl.multiple_of(q * 128, 128), 128)]
        same = lax.broadcasted_iota(jnp.int32, (128, 128), 0) == lax.broadcasted_iota(
            jnp.int32, (128, 128), 1
        )
        more = jnp.where(
            jnp.logical_and(same, inside), (1.0 - x) * (1.0 - x) - 0.0051 * (x * x), 0.0
        )
        return carry + jnp.sum(more, 0, keepdims=True)

    folded = lax.fori_loop(0, cb // 128, diagonal, folded)
    n_dev = n_row * n_col
    me = r * n_col + c
    shares[me] = folded

    def send_share(i):
        dst = (me + i) % n_dev
        ref = shares.at[me]
        return remote(ref, ref, once.at[10], once.at[11], (dst // n_col, dst % n_col))

    def each_peer(do):
        def one(i, carry):
            do(i)
            return carry

        lax.fori_loop(1, n_dev, one, 0)

    each_peer(lambda i: send_share(i).start())

    sent(a_all.at[0, pl.ds(0, (n_row - 1) * t)], once.at[2])
    sent(b_all.at[pl.ds(0, n_col - 1), pl.ds(0, t)], once.at[3])
    sent(stat_a.at[pl.ds(0, n_col - 1)], once.at[5])
    sent(stat_b.at[pl.ds(0, n_row - 1)], once.at[8])
    sent(b_all.at[:, pl.ds(0, (n_row - 1) * t)], once.at[7])
    sent(a_all.at[pl.ds(0, n_z)], once.at[4])

    def drain(zz, carry):
        whole = a_all.at[0]
        most = a_all.at[0, pl.ds(0, (n_row - 1) * t)]
        for way in range(2):
            sends = jnp.logical_and(zz <= z, can_up) if way == 0 else jnp.logical_and(zz >= z, can_down)
            cut = jnp.logical_and(n_z > 2, (z - zz if way == 0 else zz - z) == n_z - 2)

            @pl.when(jnp.logical_and(sends, jnp.logical_not(cut)))
            def _():
                sent(whole, s_line.at[way, zz])

            @pl.when(jnp.logical_and(sends, cut))
            def _():
                sent(most, s_line.at[way, zz])
                sent(a_all.at[0, pl.ds(0, t)], s_tail.at[way])

        return carry

    lax.fori_loop(0, n_z, drain, 0)

    landed(shares.at[pl.ds(0, n_dev - 1)], once.at[11])
    loss_out[...] = jnp.sum(jnp.sum(shares[...], 0), keepdims=True) / width
    sent(shares.at[pl.ds(0, n_dev - 1)], once.at[10])


def hbm(x):
    return pltpu.with_memory_space_constraint(x, pltpu.HBM)


def emit_body(pieces, x, out, sem):
    height = x.shape[0] // pieces

    def move(i):
        rows = pl.ds(i * height, height)
        return pltpu.make_async_copy(x.at[rows], out.at[rows], sem.at[i])

    for i in range(pieces):
        move(i).start()
    for i in range(pieces):
        move(i).wait()


def emit(x):
    return pl.pallas_call(
        functools.partial(emit_body, 8),
        out_shape=jax.ShapeDtypeStruct(x.shape, x.dtype),
        in_specs=[pl.BlockSpec(memory_space=pltpu.VMEM)],
        out_specs=pl.BlockSpec(memory_space=pltpu.HBM),
        scratch_shapes=[pltpu.SemaphoreType.DMA((8,))],
        compiler_params=pltpu.CompilerParams(vmem_limit_bytes=16 << 20),
        name="emit",
    )(x)


def shards(view_a, view_b):
    t, width = view_a.shape
    n_row = lax.axis_size("row")
    n_col = lax.axis_size("col")
    rb = width // n_row
    cb = width // n_col
    count = t * n_row * n_col
    n_chunk = t * n_row
    dma = pltpu.SemaphoreType.DMA
    size = 2 * (count * (rb + cb) + 2 * n_chunk * cb + 2 * t * width) + 4 * rb * cb
    product, loss = pl.pallas_call(
        functools.partial(body, n_row, n_col, width),
        out_shape=(
            jax.ShapeDtypeStruct((rb, cb), F32),
            jax.ShapeDtypeStruct((1, 1), F32),
        ),
        in_specs=[pl.BlockSpec(memory_space=pltpu.HBM)] * 2,
        out_specs=(pl.BlockSpec(memory_space=pltpu.VMEM),) * 2,
        scratch_shapes=[
            pltpu.VMEM((n_col, n_chunk, rb), BF16),
            pltpu.VMEM((n_col, n_chunk, cb), BF16),
            pltpu.VMEM((2 * n_chunk, cb), BF16),
            pltpu.VMEM((n_col, 2, rb), F32),
            pltpu.VMEM((n_row, 2, cb), F32),
            pltpu.VMEM((2, rb), F32),
            pltpu.VMEM((2, cb), F32),
            pltpu.VMEM((8, cb), F32),
            pltpu.VMEM((n_row * n_col, 1, 128), F32),
            dma((n_row,)), dma((n_col // 2,)),
            dma((2, n_col // 2)), dma((n_col // 2, n_row)), dma((n_col // 2 + n_row,)),
            dma((2,)), dma((TAIL,)), dma((TAIL,)),
            dma((n_col // 2,)), dma((12,)),
        ],
        compiler_params=pltpu.CompilerParams(
            collective_id=0, has_side_effects=True, vmem_limit_bytes=min(size + (12 << 20), 60 << 20)
        ),
        name="twins",
    )(hbm(view_a), hbm(view_b))
    return emit(product), loss.reshape(())


def solution(mesh):
    return jax.shard_map(
        shards,
        mesh=mesh,
        in_specs=(P(("row", "col"), None), P(("row", "col"), None)),
        out_specs=(P("row", "col"), P()),
        check_vma=False,
    )
```

```python
import functools

import jax
import jax.numpy as jnp
from jax import lax
from jax.experimental import pallas as pl
from jax.experimental.pallas import tpu as pltpu
from jax.sharding import PartitionSpec as P

MESH = pl.DeviceIdType.MESH
F32 = jnp.float32
BF16 = jnp.bfloat16
TAIL = 4


def body(
    n_row, n_col, width,
    a_in, b_in, out, loss_out,
    a_all, b_all, nb, stat_a, sums_a, total_a, stat_b, coef_a, coef_b, partial, shares,
    r_a, r_b, r_line, r_across, r_tail, x_tail, r_fwd, once,
):
    t = a_in.shape[0]
    rb = a_in.shape[1] // n_row
    cb = b_in.shape[1] // n_col
    count = t * n_row * n_col
    n_z = n_col // 2
    n_dev = n_row * n_col
    r = lax.axis_index("row")
    c = lax.axis_index("col")
    me = r * n_col + c
    z = c // 2
    k = c % 2
    mine = pl.ds(pl.multiple_of(r * t, t), t)

    def row_mate(i):
        return (r + i) % n_row

    def col_mate(j):
        return (c + j) % n_col

    def remote(src, dst, ss, rs, dev):
        return pltpu.make_async_remote_copy(
            src_ref=src, dst_ref=dst, send_sem=ss, recv_sem=rs, device_id=dev, device_id_type=MESH
        )

    own_a = pltpu.make_async_copy(
        a_in.at[:, pl.ds(pl.multiple_of(r * rb, rb), rb)], a_all.at[c, mine], once.at[0]
    )
    own_b = pltpu.make_async_copy(
        b_in.at[:, pl.ds(pl.multiple_of(c * cb, cb), cb)], b_all.at[c, mine], once.at[1]
    )
    own_a.start()
    own_b.start()

    barrier = pltpu.get_barrier_semaphore()

    peers = [(i, j) for i in range(n_row) for j in range(n_col) if i or j]
    peers.sort(key=lambda ij: (min(ij) > 0, ij))
    mates = [(i, j) for i, j in peers if min(i, j) == 0]
    for i, j in mates:
        pl.semaphore_signal(barrier, inc=1, device_id=(row_mate(i), col_mate(j)), device_id_type=MESH)
    pl.semaphore_wait(barrier, len(mates))

    def sent(ref, sem):
        remote(ref, ref, sem, sem, (r, c)).wait_send()

    def landed(ref, sem):
        remote(ref, ref, sem, sem, (r, c)).wait_recv()

    def send_a(i):
        dst = row_mate(i)
        cols = pl.ds(pl.multiple_of(dst * rb, rb), rb)
        return remote(a_in.at[:, cols], a_all.at[c, mine], once.at[2], r_a.at[i], (dst, c))

    def got_a(i):
        src = row_mate(n_row - i)
        rows = pl.ds(pl.multiple_of(src * t, t), t)
        return remote(a_all.at[c, rows], a_all.at[c, rows], once.at[2], r_a.at[i], (src, c))

    def send_b(j):
        dst = col_mate(j)
        cols = pl.ds(pl.multiple_of(dst * cb, cb), cb)
        return remote(b_in.at[:, cols], b_all.at[c, mine], once.at[3], r_b.at[z], (r, dst))

    for i in range(1, n_row):
        send_a(i).start()

    def block(chunk, p):
        return a_all.at[chunk, pl.ds(pl.multiple_of(p * t, t), t)]

    partner = z * 2 + (1 - k)
    above = (r, lax.min(c + 2, n_col - 2 + k))
    below = (r, lax.max(c - 2, k))
    beside = (r, partner)

    def up(chunk, p):
        ref = block(chunk, p)
        return remote(ref, ref, once.at[16], r_line.at[chunk // 2, p], above)

    def down(chunk, p):
        ref = block(chunk, p)
        return remote(ref, ref, once.at[16], r_line.at[chunk // 2, p], below)

    def across(chunk, p):
        ref = block(chunk, p)
        far = lax.max(chunk // 2 - z, z - chunk // 2) == n_z - 1
        slot = jnp.where(far, n_z + p, chunk // 2)
        return remote(ref, ref, once.at[4], r_across.at[slot], beside)

    wide = rb // TAIL

    def slab(chunk, p, f):
        return a_all.at[
            chunk, pl.ds(pl.multiple_of(p * t, t), t), pl.ds(pl.multiple_of(f * wide, wide), wide)
        ]

    def tail(way, chunk, p, f):
        ref = slab(chunk, p, f)
        return remote(ref, ref, once.at[16], r_tail.at[f], above if way == 0 else below)

    def tail_across(chunk, p, f):
        ref = slab(chunk, p, f)
        return remote(ref, ref, once.at[4], x_tail.at[f], beside)

    can_up = z < n_z - 1
    can_down = z > 0

    def slice_at(o):
        return (r + n_row - o) % n_row

    def send_line(o):
        p = slice_at(o)

        @pl.when(can_up)
        def _():
            up(c, p).start()

        @pl.when(can_down)
        def _():
            down(c, p).start()

        across(c, p).start()

    own_a.wait()
    send_line(0)

    for dist in range(n_z - 1, 0, -1):
        for side in range(2):
            zz = z - dist if side == 0 else z + dist

            @pl.when(jnp.logical_and(zz >= 0, zz < n_z))
            def _():
                for other in range(2):
                    send_b((zz * 2 + (k + other) % 2 + n_col - c) % n_col).start()

    send_b((partner + n_col - c) % n_col).start()

    for o in range(1, n_row):
        got_a(o).wait_recv()
        if o < n_row - 1:
            send_line(o)

    def moments_a(q, carry):
        cols = pl.ds(pl.multiple_of(q * 128, 128), 128)
        x = a_all[c, :, cols].astype(F32)
        stat_a[0, 0:1, cols] = jnp.sum(x, 0, keepdims=True)
        stat_a[0, 1:2, cols] = jnp.sum(x * x, 0, keepdims=True)
        return carry

    lax.fori_loop(0, rb // 128, moments_a, 0)

    half = rb // 2
    near = pl.ds(pl.multiple_of(k * half, half), half)
    away = pl.ds(pl.multiple_of((1 - k) * half, half), half)
    give_a = remote(stat_a.at[0, :, away], stat_a.at[1, :, away], once.at[5], once.at[6], beside)
    give_a.start()
    give_a.wait_send()
    landed(stat_a.at[1, :, near], once.at[6])
    sums_a[z] = stat_a[0, :, near] + stat_a[1, :, near]
    for j in range(1, n_z):
        remote(
            sums_a.at[z], sums_a.at[z], once.at[12], once.at[13], (r, (c + 2 * j) % n_col)
        ).start()
    if n_row > 1:
        send_line(n_row - 1)

    def send_fwd(i, g):
        return remote(b_all.at[g, mine], b_all.at[g, mine], once.at[7], r_fwd.at[g // 2], (row_mate(i), c))

    def each_chunk(d, do):
        for side in range(2):
            zz = z - d if side == 0 else z + d
            ok = (zz >= 0) if side == 0 else jnp.logical_and(zz < n_z, d > 0)

            @pl.when(ok)
            def _():
                do(zz * 2 + k, side)
                do(zz * 2 + (1 - k), side)

    def forward(d, carry):
        def do(g, side):
            for i in range(1, n_row):
                send_fwd(i, g).start()

        each_chunk(d, do)
        return carry

    def relay(d, o):
        split = isinstance(d, int) and d == n_z - 2 and o == n_row - 1
        from_low = z - d >= 0
        from_high = z + d < n_z
        low = (z - d) * 2 + k
        high = (z + d) * 2 + k
        p = slice_at(o)

        @pl.when(from_low)
        def _():
            up(low, p).wait_recv()

            @pl.when(can_up)
            def _():
                if split:
                    for f in range(TAIL):
                        tail(0, low, p, f).start()
                else:
                    up(low, p).start()

            across(low, p).start()

        @pl.when(from_high)
        def _():
            down(high, p).wait_recv()

            @pl.when(can_down)
            def _():
                if split:
                    for f in range(TAIL):
                        tail(1, high, p, f).start()
                else:
                    down(high, p).start()

            across(high, p).start()

    def arrive(d):
        for side in range(2):
            zz = z - d if side == 0 else z + d

            @pl.when(jnp.logical_and(zz >= 0, zz < n_z))
            def _():
                landed(b_all.at[pl.ds(zz * 2, 2), mine], r_b.at[zz])

    own_b.wait()
    landed(b_all.at[partner, mine], r_b.at[z])
    forward(0, 0)
    early = n_z > 2
    for o in range(n_row if early else 0):
        relay(1, o)
        if o + 1 < min(n_row, n_z):
            arrive(o + 1)
            forward(o + 1, 0)

    def rest(d, carry):
        arrive(d)
        forward(d, 0)
        return carry

    lax.fori_loop(min(n_row, n_z) if early else 1, n_z, rest, 0)

    for o in range(n_row if n_z > 3 else 0):
        relay(2, o)

    def moments_b(q, carry):
        cols = pl.ds(pl.multiple_of(q * 128, 128), 128)
        total = jnp.zeros((1, 128), F32)
        squares = jnp.zeros((1, 128), F32)
        for g in range(n_col):
            x = b_all[g, mine, cols].astype(F32)
            total = total + jnp.sum(x, 0, keepdims=True)
            squares = squares + jnp.sum(x * x, 0, keepdims=True)
        stat_b[r, 0:1, cols] = total
        stat_b[r, 1:2, cols] = squares
        return carry

    lax.fori_loop(0, cb // 128, moments_b, 0)

    def send_sb(i):
        return remote(stat_b.at[r], stat_b.at[r], once.at[8], once.at[9], (row_mate(i), c))

    for i in range(1, n_row):
        send_sb(i).start()

    def clear(q, carry):
        rows = pl.ds(pl.multiple_of(q * 64, 64), 64)
        out[rows, :] = jnp.zeros((64, cb), F32)
        return carry

    lax.fori_loop(0, rb // 64, clear, 0)

    landed(sums_a.at[pl.ds(0, n_z - 1)], once.at[13])
    total_a[:, near] = jnp.sum(sums_a[...], 0)
    swap_a = remote(total_a.at[:, near], total_a.at[:, near], once.at[14], once.at[15], beside)
    swap_a.start()
    landed(stat_b.at[pl.ds(0, n_row - 1)], once.at[9])

    def coefs(sums, coef):
        mean = sums[0:1] / count
        var = sums[1:2] / count - mean * mean
        coef[0:1, :] = mean
        coef[1:2, :] = lax.rsqrt(var + 1e-05)

    coefs(jnp.sum(stat_b[...], 0), coef_b)
    swap_a.wait_send()
    landed(total_a.at[:, away], once.at[15])
    coefs(total_a[...], coef_a)

    tile = min(1024, rb)

    def wait_fwd(zz):
        landed(b_all.at[pl.ds(zz * 2, 2), pl.ds(0, (n_row - 1) * t)], r_fwd.at[zz])

    def process(zz):
        landed(a_all.at[zz * 2 + (1 - k)], r_across.at[zz])
        wait_fwd(zz)
        multiply(zz, pl.ds(0, n_row * t), n_row * t)

    def normalize_b(zz, rows, height):
        def one(q, carry):
            cols = pl.ds(pl.multiple_of(q * 128, 128), 128)
            x = b_all[pl.ds(zz * 2, 2), rows, cols].astype(F32).reshape(2 * height, 128)
            nb[0 : 2 * height, cols] = ((x - coef_b[0:1, cols]) * coef_b[1:2, cols]).astype(BF16)
            return carry

        lax.fori_loop(0, cb // 128, one, 0)

    def product(zz, rows, height, cols, width):
        x = a_all[pl.ds(zz * 2, 2), rows, cols].astype(F32).reshape(2 * height, width)
        na = ((x - coef_a[0:1, cols]) * coef_a[1:2, cols]).astype(BF16)
        return lax.dot_general(
            na, nb[0 : 2 * height, :], (((0,), (0,)), ((), ())), preferred_element_type=F32
        )

    def multiply(zz, rows, height):
        normalize_b(zz, rows, height)

        def mul(q, carry):
            cols = pl.ds(pl.multiple_of(q * tile, tile), tile)
            out[cols, :] += product(zz, rows, height, cols, tile)
            return carry

        lax.fori_loop(0, rb // tile, mul, 0)

    def process_all(d):
        def one(side, carry):
            zz = jnp.where(side == 0, z - d, z + d)
            ok = jnp.logical_and(zz >= 0, zz < n_z)
            ok = jnp.logical_and(ok, jnp.logical_or(side == 0, d > 0))

            @pl.when(ok)
            def _():
                process(zz)

            return carry

        lax.fori_loop(0, 2, one, 0)

    at_end = jnp.logical_and(n_z > 2, jnp.logical_or(z == 0, z == n_z - 1))

    def finish(x):
        x = x * (1.0 / count)
        partial[...] += jnp.sum((x * x).reshape(x.shape[0] // 8, 8, cb), 0)
        return x

    def last():
        zz = jnp.where(z == 0, n_z - 1, 0)
        g = zz * 2 + k
        other = zz * 2 + (1 - k)

        @pl.when(jnp.logical_or(z == 0, z == n_z - 1))
        def _():
            wait_fwd(zz)

            def one(o, carry):
                p = slice_at(o)
                up(g, p).wait_recv()
                across(g, p).start()
                landed(block(other, p), r_across.at[n_z + p])
                multiply(zz, pl.ds(pl.multiple_of(p * t, t), t), t)
                return carry

            lax.fori_loop(0, n_row - 1 if n_z > 2 else n_row, one, 0)
            if n_z > 2:
                p = slice_at(n_row - 1)
                rows = pl.ds(pl.multiple_of(p * t, t), t)
                normalize_b(zz, rows, t)

                def take(f):
                    landed(slab(g, p, f), r_tail.at[f])
                    tail_across(g, p, f).start()

                def use(f):
                    landed(slab(other, p, f), x_tail.at[f])
                    cols = pl.ds(pl.multiple_of(f * wide, wide), wide)
                    out[cols, :] = finish(out[cols, :] + product(zz, rows, t, cols, wide))

                def some(f, carry):
                    take(f)
                    use(f - 1)
                    return carry

                take(0)
                lax.fori_loop(1, TAIL, some, 0)
                use(TAIL - 1)

    def step(d, carry):
        process_all(d)

        if n_z > 5:
            @pl.when(d + 3 < n_z - 2)
            def _():
                for o in range(n_row):
                    relay(d + 3, o)

        if n_z > 4:
            @pl.when(d + 3 == n_z - 2)
            def _():
                for o in range(n_row):
                    relay(n_z - 2, o)

        return carry

    lax.fori_loop(0, max(n_z - 1, 1), step, 0)
    partial[...] = jnp.zeros((8, cb), F32)
    if n_z > 1:
        last()

    @pl.when(jnp.logical_not(at_end))
    def _():
        def part(q, carry):
            rows = pl.ds(pl.multiple_of(q * 64, 64), 64)
            out[rows, :] = finish(out[rows, :])
            return carry

        lax.fori_loop(0, rb // 64, part, 0)

    folded = partial[:, 0:128]
    for q in range(1, cb // 128):
        folded = folded + partial[:, q * 128 : (q + 1) * 128]
    shares[me] = jnp.sum(0.0051 * folded, 0, keepdims=True)
    first = c * cb - r * rb

    @pl.when(jnp.logical_and(first > -cb, first < rb))
    def _():
        same = lax.broadcasted_iota(jnp.int32, (128, 128), 0) == lax.broadcasted_iota(
            jnp.int32, (128, 128), 1
        )

        def diagonal(q, carry):
            at = first + q * 128
            inside = jnp.logical_and(at >= 0, at < rb)
            rows = pl.ds(pl.multiple_of(jnp.where(inside, at, 0), 128), 128)
            x = out[rows, pl.ds(pl.multiple_of(q * 128, 128), 128)]
            more = (1.0 - x) * (1.0 - x) - 0.0051 * (x * x)
            return carry + jnp.where(jnp.logical_and(same, inside), more, 0.0)

        found = lax.fori_loop(0, cb // 128, diagonal, jnp.zeros((128, 128), F32))
        shares[me] += jnp.sum(found, 0, keepdims=True)


    for i, j in reversed(peers):
        remote(shares.at[me], shares.at[me], once.at[10], once.at[11], (row_mate(i), col_mate(j))).start()

    sent(a_all.at[0, pl.ds(0, (n_row - 1) * t)], once.at[2])
    sent(b_all.at[pl.ds(0, n_col - 1), pl.ds(0, t)], once.at[3])
    sent(sums_a.at[pl.ds(0, n_z - 1)], once.at[12])
    sent(stat_b.at[pl.ds(0, n_row - 1)], once.at[8])
    sent(b_all.at[:, pl.ds(0, (n_row - 1) * t)], once.at[7])
    sent(a_all.at[pl.ds(0, n_z)], once.at[4])

    ends = jnp.logical_or(z == 0, z == n_z - 1)

    @pl.when(ends)
    def _():
        sent(a_all.at[0], once.at[16])

    if n_z > 2:
        @pl.when(jnp.logical_not(ends))
        def _():
            sent(a_all.at[pl.ds(0, n_z + 1)], once.at[16])

    sent(shares.at[pl.ds(0, n_dev - 1)], once.at[10])
    landed(shares.at[pl.ds(0, n_dev - 1)], once.at[11])
    loss_out[...] = jnp.sum(jnp.sum(shares[...], 0), keepdims=True) / width


def hbm(x):
    return pltpu.with_memory_space_constraint(x, pltpu.HBM)


def emit_body(pieces, x, out, sem):
    height = x.shape[0] // pieces

    def move(i):
        rows = pl.ds(i * height, height)
        return pltpu.make_async_copy(x.at[rows], out.at[rows], sem.at[i])

    for i in range(pieces):
        move(i).start()
    for i in range(pieces):
        move(i).wait()


def emit(x):
    return pl.pallas_call(
        functools.partial(emit_body, 8),
        out_shape=jax.ShapeDtypeStruct(x.shape, x.dtype),
        in_specs=[pl.BlockSpec(memory_space=pltpu.VMEM)],
        out_specs=pl.BlockSpec(memory_space=pltpu.HBM),
        scratch_shapes=[pltpu.SemaphoreType.DMA((8,))],
        compiler_params=pltpu.CompilerParams(vmem_limit_bytes=16 << 20),
        name="emit",
    )(x)


def shards(view_a, view_b):
    t, width = view_a.shape
    n_row = lax.axis_size("row")
    n_col = lax.axis_size("col")
    rb = width // n_row
    cb = width // n_col
    count = t * n_row * n_col
    n_chunk = t * n_row
    dma = pltpu.SemaphoreType.DMA
    size = 2 * (count * (rb + cb) + 2 * n_chunk * cb + 2 * t * width) + 4 * rb * cb
    product, loss = pl.pallas_call(
        functools.partial(body, n_row, n_col, width),
        out_shape=(
            jax.ShapeDtypeStruct((rb, cb), F32),
            jax.ShapeDtypeStruct((1, 1), F32),
        ),
        in_specs=[pl.BlockSpec(memory_space=pltpu.HBM)] * 2,
        out_specs=(pl.BlockSpec(memory_space=pltpu.VMEM),) * 2,
        scratch_shapes=[
            pltpu.VMEM((n_col, n_chunk, rb), BF16),
            pltpu.VMEM((n_col, n_chunk, cb), BF16),
            pltpu.VMEM((2 * n_chunk, cb), BF16),
            pltpu.VMEM((2, 2, rb), F32),
            pltpu.VMEM((n_col // 2, 2, rb // 2), F32),
            pltpu.VMEM((2, rb), F32),
            pltpu.VMEM((n_row, 2, cb), F32),
            pltpu.VMEM((2, rb), F32),
            pltpu.VMEM((2, cb), F32),
            pltpu.VMEM((8, cb), F32),
            pltpu.VMEM((n_row * n_col, 1, 128), F32),
            dma((n_row,)), dma((n_col // 2,)),
            dma((n_col // 2, n_row)), dma((n_col // 2 + n_row,)),
            dma((TAIL,)), dma((TAIL,)),
            dma((n_col // 2,)), dma((17,)),
        ],
        compiler_params=pltpu.CompilerParams(
            collective_id=0, has_side_effects=True, vmem_limit_bytes=min(size + (12 << 20), 60 << 20)
        ),
        name="twins",
    )(hbm(view_a), hbm(view_b))
    return emit(product), loss.reshape(())


def solution(mesh):
    return jax.shard_map(
        shards,
        mesh=mesh,
        in_specs=(P(("row", "col"), None), P(("row", "col"), None)),
        out_specs=(P("row", "col"), P()),
        check_vma=False,
    )
```

```python
import functools

import jax
import jax.numpy as jnp
from jax import lax
from jax.experimental import pallas as pl
from jax.experimental.pallas import tpu as pltpu
from jax.sharding import PartitionSpec as P

MESH = pl.DeviceIdType.MESH
F32 = jnp.float32
BF16 = jnp.bfloat16
TAIL = 4


def body(
    n_row, n_col,
    a_in, b_in, out, shares_out,
    a_all, b_all, nb, stat_a, sums_a, total_a, stat_b, coef_a, coef_b, partial, shares,
    r_a, r_b, r_line, r_across, r_tail, x_tail, r_fwd, once,
):
    t = a_in.shape[0]
    rb = a_in.shape[1] // n_row
    cb = b_in.shape[1] // n_col
    count = t * n_row * n_col
    n_z = n_col // 2
    n_dev = n_row * n_col
    r = lax.axis_index("row")
    c = lax.axis_index("col")
    me = r * n_col + c
    z = c // 2
    k = c % 2
    mine = pl.ds(pl.multiple_of(r * t, t), t)

    def row_mate(i):
        return (r + i) % n_row

    def col_mate(j):
        return (c + j) % n_col

    def remote(src, dst, ss, rs, dev):
        return pltpu.make_async_remote_copy(
            src_ref=src, dst_ref=dst, send_sem=ss, recv_sem=rs, device_id=dev, device_id_type=MESH
        )

    own_a = pltpu.make_async_copy(
        a_in.at[:, pl.ds(pl.multiple_of(r * rb, rb), rb)], a_all.at[c, mine], once.at[0]
    )
    own_b = pltpu.make_async_copy(
        b_in.at[:, pl.ds(pl.multiple_of(c * cb, cb), cb)], b_all.at[c, mine], once.at[1]
    )
    own_a.start()
    own_b.start()

    barrier = pltpu.get_barrier_semaphore()

    peers = [(i, j) for i in range(n_row) for j in range(n_col) if i or j]
    peers.sort(key=lambda ij: (min(ij) > 0, ij))
    mates = [(i, j) for i, j in peers if min(i, j) == 0]
    for i, j in mates:
        pl.semaphore_signal(barrier, inc=1, device_id=(row_mate(i), col_mate(j)), device_id_type=MESH)
    pl.semaphore_wait(barrier, len(mates))

    def sent(ref, sem):
        remote(ref, ref, sem, sem, (r, c)).wait_send()

    def landed(ref, sem):
        remote(ref, ref, sem, sem, (r, c)).wait_recv()

    def send_a(i):
        dst = row_mate(i)
        cols = pl.ds(pl.multiple_of(dst * rb, rb), rb)
        return remote(a_in.at[:, cols], a_all.at[c, mine], once.at[2], r_a.at[i], (dst, c))

    def got_a(i):
        src = row_mate(n_row - i)
        rows = pl.ds(pl.multiple_of(src * t, t), t)
        return remote(a_all.at[c, rows], a_all.at[c, rows], once.at[2], r_a.at[i], (src, c))

    def send_b(j):
        dst = col_mate(j)
        cols = pl.ds(pl.multiple_of(dst * cb, cb), cb)
        return remote(b_in.at[:, cols], b_all.at[c, mine], once.at[3], r_b.at[z], (r, dst))

    def block(chunk, p):
        return a_all.at[chunk, pl.ds(pl.multiple_of(p * t, t), t)]

    partner = z * 2 + (1 - k)
    above = (r, lax.min(c + 2, n_col - 2 + k))
    below = (r, lax.max(c - 2, k))
    beside = (r, partner)

    def up(chunk, p):
        ref = block(chunk, p)
        return remote(ref, ref, once.at[16], r_line.at[chunk // 2, p], above)

    def down(chunk, p):
        ref = block(chunk, p)
        return remote(ref, ref, once.at[16], r_line.at[chunk // 2 - 1, p], below)

    def across(chunk, p):
        ref = block(chunk, p)
        far = lax.max(chunk // 2 - z, z - chunk // 2) == n_z - 1
        slot = jnp.where(far, n_z + p, chunk // 2)
        return remote(ref, ref, once.at[4], r_across.at[slot], beside)

    wide = rb // TAIL

    def slab(chunk, p, f):
        return a_all.at[
            chunk, pl.ds(pl.multiple_of(p * t, t), t), pl.ds(pl.multiple_of(f * wide, wide), wide)
        ]

    def tail(way, chunk, p, f):
        ref = slab(chunk, p, f)
        return remote(ref, ref, once.at[16], r_tail.at[f], above if way == 0 else below)

    def tail_across(chunk, p, f):
        ref = slab(chunk, p, f)
        return remote(ref, ref, once.at[4], x_tail.at[f], beside)

    can_up = z < n_z - 1
    can_down = z > 0

    def slice_at(o):
        return (r + n_row - o) % n_row

    def send_line(o):
        p = slice_at(o)

        @pl.when(can_up)
        def _():
            up(c, p).start()

        @pl.when(can_down)
        def _():
            down(c, p).start()

        across(c, p).start()

    own_a.wait()
    send_line(0)
    for i in range(1, n_row):
        send_a(i).start()

    for dist in range(n_z - 1, 0, -1):
        for side in range(2):
            zz = z - dist if side == 0 else z + dist

            @pl.when(jnp.logical_and(zz >= 0, zz < n_z))
            def _():
                for other in range(2):
                    send_b((zz * 2 + (k + other) % 2 + n_col - c) % n_col).start()

    send_b((partner + n_col - c) % n_col).start()

    for o in range(1, n_row):
        got_a(o).wait_recv()
        if o < n_row - 1:
            send_line(o)

    def moments_a(q, carry):
        cols = pl.ds(pl.multiple_of(q * 128, 128), 128)
        x = a_all[c, :, cols].astype(F32)
        stat_a[0, 0:1, cols] = jnp.sum(x, 0, keepdims=True)
        stat_a[0, 1:2, cols] = jnp.sum(x * x, 0, keepdims=True)
        return carry

    lax.fori_loop(0, rb // 128, moments_a, 0)

    half = rb // 2
    near = pl.ds(pl.multiple_of(k * half, half), half)
    away = pl.ds(pl.multiple_of((1 - k) * half, half), half)
    give_a = remote(stat_a.at[0, :, away], stat_a.at[1, :, away], once.at[5], once.at[6], beside)
    give_a.start()
    give_a.wait_send()
    landed(stat_a.at[1, :, near], once.at[6])
    sums_a[z] = stat_a[0, :, near] + stat_a[1, :, near]
    for j in range(1, n_z):
        remote(
            sums_a.at[z], sums_a.at[z], once.at[12], once.at[13], (r, (c + 2 * j) % n_col)
        ).start()
    if n_row > 1:
        send_line(n_row - 1)

    def send_fwd(i, g):
        return remote(b_all.at[g, mine], b_all.at[g, mine], once.at[7], r_fwd.at[g // 2], (row_mate(i), c))

    def each_chunk(d, do):
        for side in range(2):
            zz = z - d if side == 0 else z + d
            ok = (zz >= 0) if side == 0 else jnp.logical_and(zz < n_z, d > 0)

            @pl.when(ok)
            def _():
                do(zz * 2 + k, side)
                do(zz * 2 + (1 - k), side)

    def forward(d, carry):
        def do(g, side):
            for i in range(1, n_row):
                send_fwd(i, g).start()

        each_chunk(d, do)
        return carry

    def relay(d, o):
        split = isinstance(d, int) and d == n_z - 2 and o == n_row - 1
        from_low = z - d >= 0
        from_high = z + d < n_z
        low = (z - d) * 2 + k
        high = (z + d) * 2 + k
        p = slice_at(o)

        @pl.when(from_low)
        def _():
            up(low, p).wait_recv()

            @pl.when(can_up)
            def _():
                if split:
                    for f in range(TAIL):
                        tail(0, low, p, f).start()
                else:
                    up(low, p).start()

            across(low, p).start()

        @pl.when(from_high)
        def _():
            down(high, p).wait_recv()

            @pl.when(can_down)
            def _():
                if split:
                    for f in range(TAIL):
                        tail(1, high, p, f).start()
                else:
                    down(high, p).start()

            across(high, p).start()

    def arrive(d):
        for side in range(2):
            zz = z - d if side == 0 else z + d

            @pl.when(jnp.logical_and(zz >= 0, zz < n_z))
            def _():
                landed(b_all.at[pl.ds(zz * 2, 2), mine], r_b.at[zz])

    own_b.wait()
    landed(b_all.at[partner, mine], r_b.at[z])
    forward(0, 0)
    early = n_z > 2
    for o in range(n_row if early else 0):
        relay(1, o)
        if o + 1 < min(n_row, n_z):
            arrive(o + 1)
            forward(o + 1, 0)

    def rest(d, carry):
        arrive(d)
        forward(d, 0)
        return carry

    lax.fori_loop(min(n_row, n_z) if early else 1, n_z, rest, 0)

    for o in range(n_row if n_z > 3 else 0):
        relay(2, o)

    def moments_b(q, carry):
        cols = pl.ds(pl.multiple_of(q * 128, 128), 128)
        total = jnp.zeros((1, 128), F32)
        squares = jnp.zeros((1, 128), F32)
        for g in range(n_col):
            x = b_all[g, mine, cols].astype(F32)
            total = total + jnp.sum(x, 0, keepdims=True)
            squares = squares + jnp.sum(x * x, 0, keepdims=True)
        stat_b[r, 0:1, cols] = total
        stat_b[r, 1:2, cols] = squares
        return carry

    lax.fori_loop(0, cb // 128, moments_b, 0)

    def send_sb(i):
        return remote(stat_b.at[r], stat_b.at[r], once.at[8], once.at[9], (row_mate(i), c))

    for i in range(1, n_row):
        send_sb(i).start()

    def clear(q, carry):
        rows = pl.ds(pl.multiple_of(q * 64, 64), 64)
        out[rows, :] = jnp.zeros((64, cb), F32)
        return carry

    lax.fori_loop(0, rb // 64, clear, 0)

    landed(sums_a.at[pl.ds(0, n_z - 1)], once.at[13])
    total_a[:, near] = jnp.sum(sums_a[...], 0)
    swap_a = remote(total_a.at[:, near], total_a.at[:, near], once.at[14], once.at[15], beside)
    swap_a.start()
    landed(stat_b.at[pl.ds(0, n_row - 1)], once.at[9])

    def coefs(sums, coef):
        mean = sums[0:1] / count
        var = sums[1:2] / count - mean * mean
        coef[0:1, :] = mean
        coef[1:2, :] = lax.rsqrt(var + 1e-05)

    coefs(jnp.sum(stat_b[...], 0), coef_b)
    swap_a.wait_send()
    landed(total_a.at[:, away], once.at[15])
    coefs(total_a[...], coef_a)

    tile = min(1024, rb)

    def wait_fwd(zz):
        landed(b_all.at[pl.ds(zz * 2, 2), pl.ds(0, (n_row - 1) * t)], r_fwd.at[zz])

    def process(zz):
        landed(a_all.at[zz * 2 + (1 - k)], r_across.at[zz])
        wait_fwd(zz)
        multiply(zz, pl.ds(0, n_row * t), n_row * t)

    def normalize_b(zz, rows, height):
        def one(q, carry):
            cols = pl.ds(pl.multiple_of(q * 128, 128), 128)
            x = b_all[pl.ds(zz * 2, 2), rows, cols].astype(F32).reshape(2 * height, 128)
            nb[0 : 2 * height, cols] = ((x - coef_b[0:1, cols]) * coef_b[1:2, cols]).astype(BF16)
            return carry

        lax.fori_loop(0, cb // 128, one, 0)

    def product(zz, rows, height, cols, width):
        x = a_all[pl.ds(zz * 2, 2), rows, cols].astype(F32).reshape(2 * height, width)
        na = ((x - coef_a[0:1, cols]) * coef_a[1:2, cols]).astype(BF16)
        return lax.dot_general(
            na, nb[0 : 2 * height, :], (((0,), (0,)), ((), ())), preferred_element_type=F32
        )

    def multiply(zz, rows, height):
        normalize_b(zz, rows, height)

        def mul(q, carry):
            cols = pl.ds(pl.multiple_of(q * tile, tile), tile)
            out[cols, :] += product(zz, rows, height, cols, tile)
            return carry

        lax.fori_loop(0, rb // tile, mul, 0)

    def process_all(d):
        def one(side, carry):
            zz = jnp.where(side == 0, z - d, z + d)
            ok = jnp.logical_and(zz >= 0, zz < n_z)
            ok = jnp.logical_and(ok, jnp.logical_or(side == 0, d > 0))

            @pl.when(ok)
            def _():
                process(zz)

            return carry

        lax.fori_loop(0, 2, one, 0)

    at_end = jnp.logical_and(n_z > 2, jnp.logical_or(z == 0, z == n_z - 1))

    def finish(x):
        x = x * (1.0 / count)
        partial[...] += jnp.sum((x * x).reshape(x.shape[0] // 8, 8, cb), 0)
        return x

    def last():
        zz = jnp.where(z == 0, n_z - 1, 0)
        g = zz * 2 + k
        other = zz * 2 + (1 - k)

        @pl.when(jnp.logical_or(z == 0, z == n_z - 1))
        def _():
            wait_fwd(zz)

            def one(o, carry):
                p = slice_at(o)
                landed(block(g, p), r_line.at[jnp.where(z == 0, n_z - 2, 0), p])
                across(g, p).start()
                landed(block(other, p), r_across.at[n_z + p])
                multiply(zz, pl.ds(pl.multiple_of(p * t, t), t), t)
                return carry

            lax.fori_loop(0, n_row - 1 if n_z > 2 else n_row, one, 0)
            if n_z > 2:
                p = slice_at(n_row - 1)
                rows = pl.ds(pl.multiple_of(p * t, t), t)
                normalize_b(zz, rows, t)

                def take(f):
                    landed(slab(g, p, f), r_tail.at[f])
                    tail_across(g, p, f).start()

                def use(f):
                    landed(slab(other, p, f), x_tail.at[f])
                    cols = pl.ds(pl.multiple_of(f * wide, wide), wide)
                    out[cols, :] = finish(out[cols, :] + product(zz, rows, t, cols, wide))

                def some(f, carry):
                    take(f)
                    use(f - 1)
                    return carry

                take(0)
                lax.fori_loop(1, TAIL, some, 0)
                use(TAIL - 1)

    def step(d, carry):
        process_all(d)

        if n_z > 5:
            @pl.when(d + 3 < n_z - 2)
            def _():
                for o in range(n_row):
                    relay(d + 3, o)

        if n_z > 4:
            @pl.when(d + 3 == n_z - 2)
            def _():
                for o in range(n_row):
                    relay(n_z - 2, o)

        return carry

    lax.fori_loop(0, max(n_z - 1, 1), step, 0)
    partial[...] = jnp.zeros((8, cb), F32)
    if n_z > 1:
        last()

    @pl.when(jnp.logical_not(at_end))
    def _():
        def part(q, carry):
            rows = pl.ds(pl.multiple_of(q * 64, 64), 64)
            out[rows, :] = finish(out[rows, :])
            return carry

        lax.fori_loop(0, rb // 64, part, 0)

    folded = partial[:, 0:128]
    for q in range(1, cb // 128):
        folded = folded + partial[:, q * 128 : (q + 1) * 128]
    shares[me] = jnp.sum(0.0051 * folded, 0, keepdims=True)
    first = c * cb - r * rb

    @pl.when(jnp.logical_and(first > -cb, first < rb))
    def _():
        same = lax.broadcasted_iota(jnp.int32, (128, 128), 0) == lax.broadcasted_iota(
            jnp.int32, (128, 128), 1
        )

        def diagonal(q, carry):
            at = first + q * 128
            inside = jnp.logical_and(at >= 0, at < rb)
            rows = pl.ds(pl.multiple_of(jnp.where(inside, at, 0), 128), 128)
            x = out[rows, pl.ds(pl.multiple_of(q * 128, 128), 128)]
            more = (1.0 - x) * (1.0 - x) - 0.0051 * (x * x)
            return carry + jnp.where(jnp.logical_and(same, inside), more, 0.0)

        found = lax.fori_loop(0, cb // 128, diagonal, jnp.zeros((128, 128), F32))
        shares[me] += jnp.sum(found, 0, keepdims=True)


    way = jnp.where(2 * z >= n_z, 1, n_col - 1)
    far_first = sorted(peers, key=lambda ij: (ij[1] == 0, (ij[1] - 2) % n_col, ij[0] % 2 == 0))
    for i, j in far_first:
        to = (row_mate(i), (c + way * j) % n_col)
        remote(shares.at[me], shares.at[me], once.at[10], once.at[11], to).start()

    sent(a_all.at[0, pl.ds(0, (n_row - 1) * t)], once.at[2])
    sent(b_all.at[pl.ds(0, n_col - 1), pl.ds(0, t)], once.at[3])
    sent(sums_a.at[pl.ds(0, n_z - 1)], once.at[12])
    sent(stat_b.at[pl.ds(0, n_row - 1)], once.at[8])
    sent(b_all.at[:, pl.ds(0, (n_row - 1) * t)], once.at[7])
    sent(a_all.at[pl.ds(0, n_z)], once.at[4])

    ends = jnp.logical_or(z == 0, z == n_z - 1)

    @pl.when(ends)
    def _():
        sent(a_all.at[0], once.at[16])

    if n_z > 2:
        @pl.when(jnp.logical_not(ends))
        def _():
            sent(a_all.at[pl.ds(0, n_z + 1)], once.at[16])

    sent(shares.at[pl.ds(0, n_dev - 1)], once.at[10])
    landed(shares.at[pl.ds(0, n_dev - 1)], once.at[11])
    shares_out[...] = shares[...]


def hbm(x):
    return pltpu.with_memory_space_constraint(x, pltpu.HBM)


def emit_body(pieces, width, x, shares, out, loss_out, loss, sem):
    height = x.shape[0] // pieces
    for i in range(pieces):
        rows = pl.ds(i * height, height)
        pltpu.make_async_copy(x.at[rows], out.at[rows], sem.at[0]).start()
    loss[...] = jnp.sum(jnp.sum(shares[...], 0), keepdims=True) / width
    send_loss = pltpu.make_async_copy(loss, loss_out, sem.at[1])
    send_loss.start()
    pltpu.make_async_copy(x, out, sem.at[0]).wait()
    send_loss.wait()


def emit(x, shares, width):
    return pl.pallas_call(
        functools.partial(emit_body, 8, width),
        out_shape=(jax.ShapeDtypeStruct(x.shape, x.dtype), jax.ShapeDtypeStruct((1, 1), F32)),
        in_specs=[pl.BlockSpec(memory_space=pltpu.VMEM)] * 2,
        out_specs=(pl.BlockSpec(memory_space=pltpu.HBM),) * 2,
        scratch_shapes=[pltpu.VMEM((1, 1), F32), pltpu.SemaphoreType.DMA((2,))],
        compiler_params=pltpu.CompilerParams(vmem_limit_bytes=16 << 20),
        name="emit",
    )(x, shares)


def shards(view_a, view_b):
    t, width = view_a.shape
    n_row = lax.axis_size("row")
    n_col = lax.axis_size("col")
    rb = width // n_row
    cb = width // n_col
    count = t * n_row * n_col
    n_chunk = t * n_row
    dma = pltpu.SemaphoreType.DMA
    size = 2 * (count * (rb + cb) + 2 * n_chunk * cb + 2 * t * width) + 4 * rb * cb
    product, shares = pl.pallas_call(
        functools.partial(body, n_row, n_col),
        out_shape=(
            jax.ShapeDtypeStruct((rb, cb), F32),
            jax.ShapeDtypeStruct((n_row * n_col, 1, 128), F32),
        ),
        in_specs=[pl.BlockSpec(memory_space=pltpu.HBM)] * 2,
        out_specs=(pl.BlockSpec(memory_space=pltpu.VMEM),) * 2,
        scratch_shapes=[
            pltpu.VMEM((n_col, n_chunk, rb), BF16),
            pltpu.VMEM((n_col, n_chunk, cb), BF16),
            pltpu.VMEM((2 * n_chunk, cb), BF16),
            pltpu.VMEM((2, 2, rb), F32),
            pltpu.VMEM((n_col // 2, 2, rb // 2), F32),
            pltpu.VMEM((2, rb), F32),
            pltpu.VMEM((n_row, 2, cb), F32),
            pltpu.VMEM((2, rb), F32),
            pltpu.VMEM((2, cb), F32),
            pltpu.VMEM((8, cb), F32),
            pltpu.VMEM((n_row * n_col, 1, 128), F32),
            dma((n_row,)), dma((n_col // 2,)),
            dma((max(n_col // 2 - 1, 1), n_row)), dma((n_col // 2 + n_row,)),
            dma((TAIL,)), dma((TAIL,)),
            dma((n_col // 2,)), dma((17,)),
        ],
        compiler_params=pltpu.CompilerParams(
            collective_id=0, has_side_effects=True, vmem_limit_bytes=min(size + (12 << 20), 60 << 20)
        ),
        name="twins",
    )(hbm(view_a), hbm(view_b))
    product, loss = emit(product, shares, width)
    return product, loss.reshape(())


def solution(mesh):
    return jax.shard_map(
        shards,
        mesh=mesh,
        in_specs=(P(("row", "col"), None), P(("row", "col"), None)),
        out_specs=(P("row", "col"), P()),
        check_vma=False,
    )
```

```python
import functools

import jax
import jax.numpy as jnp
from jax import lax
from jax.experimental import pallas as pl
from jax.experimental.pallas import tpu as pltpu
from jax.sharding import PartitionSpec as P

MESH = pl.DeviceIdType.MESH
F32 = jnp.float32
BF16 = jnp.bfloat16
TAIL = 4


def body(
    n_row, n_col,
    a_in, b_in, out, shares_out,
    a_all, b_all, nb, stat_a, sums_a, total_a, stat_b, coef_a, coef_b, partial, spread, shares,
    r_a, r_b, r_line, r_across, r_tail, x_tail, r_fwd, once,
):
    t = a_in.shape[0]
    rb = a_in.shape[1] // n_row
    cb = b_in.shape[1] // n_col
    count = t * n_row * n_col
    n_z = n_col // 2
    n_dev = n_row * n_col
    r = lax.axis_index("row")
    c = lax.axis_index("col")
    me = r * n_col + c
    z = c // 2
    k = c % 2
    mine = pl.ds(pl.multiple_of(r * t, t), t)

    def row_mate(i):
        return (r + i) % n_row

    def col_mate(j):
        return (c + j) % n_col

    def remote(src, dst, ss, rs, dev):
        return pltpu.make_async_remote_copy(
            src_ref=src, dst_ref=dst, send_sem=ss, recv_sem=rs, device_id=dev, device_id_type=MESH
        )

    own_a = pltpu.make_async_copy(
        a_in.at[:, pl.ds(pl.multiple_of(r * rb, rb), rb)], a_all.at[c, mine], once.at[0]
    )
    own_b = pltpu.make_async_copy(
        b_in.at[:, pl.ds(pl.multiple_of(c * cb, cb), cb)], b_all.at[c, mine], once.at[1]
    )
    own_a.start()
    own_b.start()

    barrier = pltpu.get_barrier_semaphore()

    peers = [(i, j) for i in range(n_row) for j in range(n_col) if i or j]
    peers.sort(key=lambda ij: (min(ij) > 0, ij))
    mates = [(i, j) for i, j in peers if min(i, j) == 0]
    for i, j in mates:
        pl.semaphore_signal(barrier, inc=1, device_id=(row_mate(i), col_mate(j)), device_id_type=MESH)
    pl.semaphore_wait(barrier, len(mates))

    def sent(ref, sem):
        remote(ref, ref, sem, sem, (r, c)).wait_send()

    def landed(ref, sem):
        remote(ref, ref, sem, sem, (r, c)).wait_recv()

    def send_a(i):
        dst = row_mate(i)
        cols = pl.ds(pl.multiple_of(dst * rb, rb), rb)
        return remote(a_in.at[:, cols], a_all.at[c, mine], once.at[2], r_a.at[i], (dst, c))

    def got_a(i):
        src = row_mate(n_row - i)
        rows = pl.ds(pl.multiple_of(src * t, t), t)
        return remote(a_all.at[c, rows], a_all.at[c, rows], once.at[2], r_a.at[i], (src, c))

    def send_b(j):
        dst = col_mate(j)
        cols = pl.ds(pl.multiple_of(dst * cb, cb), cb)
        return remote(b_in.at[:, cols], b_all.at[c, mine], once.at[3], r_b.at[z], (r, dst))

    def block(chunk, p):
        return a_all.at[chunk, pl.ds(pl.multiple_of(p * t, t), t)]

    partner = z * 2 + (1 - k)
    above = (r, lax.min(c + 2, n_col - 2 + k))
    below = (r, lax.max(c - 2, k))
    beside = (r, partner)

    def up(chunk, p):
        ref = block(chunk, p)
        return remote(ref, ref, once.at[16], r_line.at[chunk // 2, p], above)

    def down(chunk, p):
        ref = block(chunk, p)
        return remote(ref, ref, once.at[16], r_line.at[chunk // 2 - 1, p], below)

    def across(chunk, p):
        ref = block(chunk, p)
        far = lax.max(chunk // 2 - z, z - chunk // 2) == n_z - 1
        slot = jnp.where(far, n_z + p, chunk // 2)
        return remote(ref, ref, once.at[4], r_across.at[slot], beside)

    widths = [rb >> min(f + 1, TAIL - 1) for f in range(TAIL)]
    slabs = [pl.ds(sum(widths[:f]), widths[f]) for f in range(TAIL)]

    def slab(chunk, p, f):
        return a_all.at[chunk, pl.ds(pl.multiple_of(p * t, t), t), slabs[f]]

    def tail(way, chunk, p, f):
        ref = slab(chunk, p, f)
        return remote(ref, ref, once.at[16], r_tail.at[f], above if way == 0 else below)

    def tail_across(chunk, p, f):
        ref = slab(chunk, p, f)
        return remote(ref, ref, once.at[4], x_tail.at[f], beside)

    can_up = z < n_z - 1
    can_down = z > 0

    def slice_at(o):
        return (r + n_row - o) % n_row

    def send_line(o):
        p = slice_at(o)

        @pl.when(can_up)
        def _():
            up(c, p).start()

        @pl.when(can_down)
        def _():
            down(c, p).start()

        across(c, p).start()

    own_a.wait()
    send_line(0)
    for i in range(1, n_row):
        send_a(i).start()

    for dist in range(n_z - 1, 0, -1):
        for side in range(2):
            zz = z - dist if side == 0 else z + dist

            @pl.when(jnp.logical_and(zz >= 0, zz < n_z))
            def _():
                for other in range(2):
                    send_b((zz * 2 + (k + other) % 2 + n_col - c) % n_col).start()

    send_b((partner + n_col - c) % n_col).start()

    for o in range(1, n_row):
        got_a(o).wait_recv()
        if o < n_row - 1:
            send_line(o)

    def moments_a(q, carry):
        cols = pl.ds(pl.multiple_of(q * 128, 128), 128)
        x = a_all[c, :, cols].astype(F32)
        stat_a[0, 0:1, cols] = jnp.sum(x, 0, keepdims=True)
        stat_a[0, 1:2, cols] = jnp.sum(x * x, 0, keepdims=True)
        return carry

    lax.fori_loop(0, rb // 128, moments_a, 0)

    half = rb // 2
    near = pl.ds(pl.multiple_of(k * half, half), half)
    away = pl.ds(pl.multiple_of((1 - k) * half, half), half)
    give_a = remote(stat_a.at[0, :, away], stat_a.at[1, :, away], once.at[5], once.at[6], beside)
    give_a.start()
    give_a.wait_send()
    landed(stat_a.at[1, :, near], once.at[6])
    sums_a[z] = stat_a[0, :, near] + stat_a[1, :, near]
    for j in range(1, n_z):
        remote(
            sums_a.at[z], sums_a.at[z], once.at[12], once.at[13], (r, (c + 2 * j) % n_col)
        ).start()
    if n_row > 1:
        send_line(n_row - 1)

    def send_fwd(i, g):
        return remote(b_all.at[g, mine], b_all.at[g, mine], once.at[7], r_fwd.at[g // 2], (row_mate(i), c))

    def each_chunk(d, do):
        for side in range(2):
            zz = z - d if side == 0 else z + d
            ok = (zz >= 0) if side == 0 else jnp.logical_and(zz < n_z, d > 0)

            @pl.when(ok)
            def _():
                do(zz * 2 + k, side)
                do(zz * 2 + (1 - k), side)

    def forward(d, carry):
        def do(g, side):
            for i in range(1, n_row):
                send_fwd(i, g).start()

        each_chunk(d, do)
        return carry

    def relay(d, o):
        split = isinstance(d, int) and d == n_z - 2 and o == n_row - 1
        from_low = z - d >= 0
        from_high = z + d < n_z
        low = (z - d) * 2 + k
        high = (z + d) * 2 + k
        p = slice_at(o)

        @pl.when(from_low)
        def _():
            up(low, p).wait_recv()

            @pl.when(can_up)
            def _():
                if split:
                    for f in range(TAIL):
                        tail(0, low, p, f).start()
                else:
                    up(low, p).start()

            across(low, p).start()

        @pl.when(from_high)
        def _():
            down(high, p).wait_recv()

            @pl.when(can_down)
            def _():
                if split:
                    for f in range(TAIL):
                        tail(1, high, p, f).start()
                else:
                    down(high, p).start()

            across(high, p).start()

    def arrive(d):
        for side in range(2):
            zz = z - d if side == 0 else z + d

            @pl.when(jnp.logical_and(zz >= 0, zz < n_z))
            def _():
                landed(b_all.at[pl.ds(zz * 2, 2), mine], r_b.at[zz])

    own_b.wait()
    landed(b_all.at[partner, mine], r_b.at[z])
    forward(0, 0)
    early = n_z > 2
    for o in range(n_row if early else 0):
        relay(1, o)
        if o + 1 < min(n_row, n_z):
            arrive(o + 1)
            forward(o + 1, 0)

    def rest(d, carry):
        arrive(d)
        forward(d, 0)
        return carry

    lax.fori_loop(min(n_row, n_z) if early else 1, n_z, rest, 0)

    for o in range(n_row if n_z > 3 else 0):
        relay(2, o)

    def moments_b(q, carry):
        cols = pl.ds(pl.multiple_of(q * 128, 128), 128)
        total = jnp.zeros((1, 128), F32)
        squares = jnp.zeros((1, 128), F32)
        for g in range(n_col):
            x = b_all[g, mine, cols].astype(F32)
            total = total + jnp.sum(x, 0, keepdims=True)
            squares = squares + jnp.sum(x * x, 0, keepdims=True)
        stat_b[r, 0:1, cols] = total
        stat_b[r, 1:2, cols] = squares
        return carry

    lax.fori_loop(0, cb // 128, moments_b, 0)

    def send_sb(i):
        return remote(stat_b.at[r], stat_b.at[r], once.at[8], once.at[9], (row_mate(i), c))

    for i in range(1, n_row):
        send_sb(i).start()

    def clear(q, carry):
        rows = pl.ds(pl.multiple_of(q * 64, 64), 64)
        out[rows, :] = jnp.zeros((64, cb), F32)
        return carry

    lax.fori_loop(0, rb // 64, clear, 0)

    landed(sums_a.at[pl.ds(0, n_z - 1)], once.at[13])
    total_a[:, near] = jnp.sum(sums_a[...], 0)
    swap_a = remote(total_a.at[:, near], total_a.at[:, near], once.at[14], once.at[15], beside)
    swap_a.start()
    landed(stat_b.at[pl.ds(0, n_row - 1)], once.at[9])

    def coefs(sums, coef):
        mean = sums[0:1] / count
        var = sums[1:2] / count - mean * mean
        coef[0:1, :] = mean
        coef[1:2, :] = lax.rsqrt(var + 1e-05)

    coefs(jnp.sum(stat_b[...], 0), coef_b)
    swap_a.wait_send()
    landed(total_a.at[:, away], once.at[15])
    coefs(total_a[...], coef_a)

    tile = min(1024, rb)

    def wait_fwd(zz):
        landed(b_all.at[pl.ds(zz * 2, 2), pl.ds(0, (n_row - 1) * t)], r_fwd.at[zz])

    def process(zz):
        landed(a_all.at[zz * 2 + (1 - k)], r_across.at[zz])
        wait_fwd(zz)
        multiply(zz, pl.ds(0, n_row * t), n_row * t)

    def normalize_b(zz, rows, height):
        def one(q, carry):
            cols = pl.ds(pl.multiple_of(q * 128, 128), 128)
            x = b_all[pl.ds(zz * 2, 2), rows, cols].astype(F32).reshape(2 * height, 128)
            nb[0 : 2 * height, cols] = ((x - coef_b[0:1, cols]) * coef_b[1:2, cols]).astype(BF16)
            return carry

        lax.fori_loop(0, cb // 128, one, 0)

    def product(zz, rows, height, cols, width):
        x = a_all[pl.ds(zz * 2, 2), rows, cols].astype(F32).reshape(2 * height, width)
        na = ((x - coef_a[0:1, cols]) * coef_a[1:2, cols]).astype(BF16)
        return lax.dot_general(
            na, nb[0 : 2 * height, :], (((0,), (0,)), ((), ())), preferred_element_type=F32
        )

    def multiply(zz, rows, height):
        normalize_b(zz, rows, height)

        def mul(q, carry):
            cols = pl.ds(pl.multiple_of(q * tile, tile), tile)
            out[cols, :] += product(zz, rows, height, cols, tile)
            return carry

        lax.fori_loop(0, rb // tile, mul, 0)

    def process_all(d):
        def one(side, carry):
            zz = jnp.where(side == 0, z - d, z + d)
            ok = jnp.logical_and(zz >= 0, zz < n_z)
            ok = jnp.logical_and(ok, jnp.logical_or(side == 0, d > 0))

            @pl.when(ok)
            def _():
                process(zz)

            return carry

        lax.fori_loop(0, 2, one, 0)

    at_end = jnp.logical_and(n_z > 2, jnp.logical_or(z == 0, z == n_z - 1))

    def finish(x):
        x = x * (1.0 / count)
        partial[...] += jnp.sum((x * x).reshape(x.shape[0] // 8, 8, cb), 0)
        return x

    first = c * cb - r * rb

    def diagonal(start, height):
        @pl.when(jnp.logical_and(first > start - cb, first < start + height))
        def _():
            same = lax.broadcasted_iota(jnp.int32, (128, 128), 0) == lax.broadcasted_iota(
                jnp.int32, (128, 128), 1
            )

            def one(q, carry):
                row = start + q * 128
                col = row - first
                inside = jnp.logical_and(col >= 0, col < cb)
                cols = pl.ds(pl.multiple_of(jnp.where(inside, col, 0), 128), 128)
                x = out[pl.ds(pl.multiple_of(row, 128), 128), cols]
                more = (1.0 - x) * (1.0 - x) - 0.0051 * (x * x)
                more = jnp.where(jnp.logical_and(same, inside), more, 0.0)
                return carry + jnp.sum(more.reshape(16, 8, 128), 0)

            spread[...] += lax.fori_loop(0, height // 128, one, jnp.zeros((8, 128), F32))

    def last():
        zz = jnp.where(z == 0, n_z - 1, 0)
        g = zz * 2 + k
        other = zz * 2 + (1 - k)

        @pl.when(jnp.logical_or(z == 0, z == n_z - 1))
        def _():
            wait_fwd(zz)

            def one(o, carry):
                p = slice_at(o)
                landed(block(g, p), r_line.at[jnp.where(z == 0, n_z - 2, 0), p])
                across(g, p).start()
                landed(block(other, p), r_across.at[n_z + p])
                multiply(zz, pl.ds(pl.multiple_of(p * t, t), t), t)
                return carry

            lax.fori_loop(0, n_row - 1 if n_z > 2 else n_row, one, 0)
            if n_z > 2:
                p = slice_at(n_row - 1)
                rows = pl.ds(pl.multiple_of(p * t, t), t)
                normalize_b(zz, rows, t)

                def take(f):
                    landed(slab(g, p, f), r_tail.at[f])
                    tail_across(g, p, f).start()

                def use(f):
                    landed(slab(other, p, f), x_tail.at[f])
                    cols = slabs[f]
                    out[cols, :] = finish(out[cols, :] + product(zz, rows, t, cols, widths[f]))
                    diagonal(slabs[f].start, widths[f])

                take(0)
                for f in range(1, TAIL):
                    take(f)
                    use(f - 1)
                use(TAIL - 1)

    def step(d, carry):
        process_all(d)

        if n_z > 5:
            @pl.when(d + 3 < n_z - 2)
            def _():
                for o in range(n_row):
                    relay(d + 3, o)

        if n_z > 4:
            @pl.when(d + 3 == n_z - 2)
            def _():
                for o in range(n_row):
                    relay(n_z - 2, o)

        return carry

    lax.fori_loop(0, max(n_z - 1, 1), step, 0)
    partial[...] = jnp.zeros((8, cb), F32)
    spread[...] = jnp.zeros((8, 128), F32)
    if n_z > 1:
        last()

    @pl.when(jnp.logical_not(at_end))
    def _():
        def part(q, carry):
            rows = pl.ds(pl.multiple_of(q * 64, 64), 64)
            out[rows, :] = finish(out[rows, :])
            return carry

        lax.fori_loop(0, rb // 64, part, 0)
        diagonal(0, rb)

    folded = partial[:, 0:128]
    for q in range(1, cb // 128):
        folded = folded + partial[:, q * 128 : (q + 1) * 128]
    shares[me] = jnp.sum(0.0051 * folded + spread[...], 0, keepdims=True)

    way = jnp.where(2 * z >= n_z, 1, n_col - 1)
    far_first = sorted(peers, key=lambda ij: (ij[1] == 0, (ij[1] - 2) % n_col, ij[0] % 2 == 0))
    for i, j in far_first:
        to = (row_mate(i), (c + way * j) % n_col)
        remote(shares.at[me], shares.at[me], once.at[10], once.at[11], to).start()

    sent(a_all.at[0, pl.ds(0, (n_row - 1) * t)], once.at[2])
    sent(b_all.at[pl.ds(0, n_col - 1), pl.ds(0, t)], once.at[3])
    sent(sums_a.at[pl.ds(0, n_z - 1)], once.at[12])
    sent(stat_b.at[pl.ds(0, n_row - 1)], once.at[8])
    sent(b_all.at[:, pl.ds(0, (n_row - 1) * t)], once.at[7])
    sent(a_all.at[pl.ds(0, n_z)], once.at[4])

    ends = jnp.logical_or(z == 0, z == n_z - 1)

    @pl.when(ends)
    def _():
        sent(a_all.at[0], once.at[16])

    if n_z > 2:
        @pl.when(jnp.logical_not(ends))
        def _():
            sent(a_all.at[pl.ds(0, n_z + 1)], once.at[16])

    sent(shares.at[pl.ds(0, n_dev - 1)], once.at[10])
    landed(shares.at[pl.ds(0, n_dev - 1)], once.at[11])
    shares_out[...] = shares[...]


def hbm(x):
    return pltpu.with_memory_space_constraint(x, pltpu.HBM)


def emit_body(pieces, width, x, shares, out, loss_out, loss, sem):
    height = x.shape[0] // pieces
    for i in range(pieces):
        rows = pl.ds(i * height, height)
        pltpu.make_async_copy(x.at[rows], out.at[rows], sem.at[0]).start()
    loss[...] = jnp.sum(jnp.sum(shares[...], 0), keepdims=True) / width
    send_loss = pltpu.make_async_copy(loss, loss_out, sem.at[1])
    send_loss.start()
    pltpu.make_async_copy(x, out, sem.at[0]).wait()
    send_loss.wait()


def emit(x, shares, width):
    return pl.pallas_call(
        functools.partial(emit_body, 8, width),
        out_shape=(jax.ShapeDtypeStruct(x.shape, x.dtype), jax.ShapeDtypeStruct((1, 1), F32)),
        in_specs=[pl.BlockSpec(memory_space=pltpu.VMEM)] * 2,
        out_specs=(pl.BlockSpec(memory_space=pltpu.HBM),) * 2,
        scratch_shapes=[pltpu.VMEM((1, 1), F32), pltpu.SemaphoreType.DMA((2,))],
        compiler_params=pltpu.CompilerParams(vmem_limit_bytes=16 << 20),
        name="emit",
    )(x, shares)


def shards(view_a, view_b):
    t, width = view_a.shape
    n_row = lax.axis_size("row")
    n_col = lax.axis_size("col")
    rb = width // n_row
    cb = width // n_col
    count = t * n_row * n_col
    n_chunk = t * n_row
    dma = pltpu.SemaphoreType.DMA
    size = 2 * (count * (rb + cb) + 2 * n_chunk * cb + 2 * t * width) + 4 * rb * cb
    product, shares = pl.pallas_call(
        functools.partial(body, n_row, n_col),
        out_shape=(
            jax.ShapeDtypeStruct((rb, cb), F32),
            jax.ShapeDtypeStruct((n_row * n_col, 1, 128), F32),
        ),
        in_specs=[pl.BlockSpec(memory_space=pltpu.HBM)] * 2,
        out_specs=(pl.BlockSpec(memory_space=pltpu.VMEM),) * 2,
        scratch_shapes=[
            pltpu.VMEM((n_col, n_chunk, rb), BF16),
            pltpu.VMEM((n_col, n_chunk, cb), BF16),
            pltpu.VMEM((2 * n_chunk, cb), BF16),
            pltpu.VMEM((2, 2, rb), F32),
            pltpu.VMEM((n_col // 2, 2, rb // 2), F32),
            pltpu.VMEM((2, rb), F32),
            pltpu.VMEM((n_row, 2, cb), F32),
            pltpu.VMEM((2, rb), F32),
            pltpu.VMEM((2, cb), F32),
            pltpu.VMEM((8, cb), F32),
            pltpu.VMEM((8, 128), F32),
            pltpu.VMEM((n_row * n_col, 1, 128), F32),
            dma((n_row,)), dma((n_col // 2,)),
            dma((max(n_col // 2 - 1, 1), n_row)), dma((n_col // 2 + n_row,)),
            dma((TAIL,)), dma((TAIL,)),
            dma((n_col // 2,)), dma((17,)),
        ],
        compiler_params=pltpu.CompilerParams(
            collective_id=0, has_side_effects=True, vmem_limit_bytes=min(size + (12 << 20), 60 << 20)
        ),
        name="twins",
    )(hbm(view_a), hbm(view_b))
    product, loss = emit(product, shares, width)
    return product, loss.reshape(())


def solution(mesh):
    return jax.shard_map(
        shards,
        mesh=mesh,
        in_specs=(P(("row", "col"), None), P(("row", "col"), None)),
        out_specs=(P("row", "col"), P()),
        check_vma=False,
    )
```

```python
import functools

import jax
import jax.numpy as jnp
from jax import lax
from jax.experimental import pallas as pl
from jax.experimental.pallas import tpu as pltpu
from jax.sharding import PartitionSpec as P

MESH = pl.DeviceIdType.MESH
F32 = jnp.float32
BF16 = jnp.bfloat16
TAIL = 4


def body(
    n_row, n_col,
    a_in, b_in, out, shares_out,
    a_all, b_all, nb, stat_a, sums_a, total_a, stat_b, coef_a, coef_b, partial, spread, shares,
    r_a, r_b, r_line, r_across, r_tail, x_tail, r_fwd, once,
):
    t = a_in.shape[0]
    rb = a_in.shape[1] // n_row
    cb = b_in.shape[1] // n_col
    count = t * n_row * n_col
    n_z = n_col // 2
    n_dev = n_row * n_col
    r = lax.axis_index("row")
    c = lax.axis_index("col")
    me = r * n_col + c
    z = c // 2
    k = c % 2
    mine = pl.ds(pl.multiple_of(r * t, t), t)

    def row_mate(i):
        return (r + i) % n_row

    def col_mate(j):
        return (c + j) % n_col

    def remote(src, dst, ss, rs, dev):
        return pltpu.make_async_remote_copy(
            src_ref=src, dst_ref=dst, send_sem=ss, recv_sem=rs, device_id=dev, device_id_type=MESH
        )

    own_a = pltpu.make_async_copy(
        a_in.at[:, pl.ds(pl.multiple_of(r * rb, rb), rb)], a_all.at[c, mine], once.at[0]
    )
    own_b = pltpu.make_async_copy(
        b_in.at[:, pl.ds(pl.multiple_of(c * cb, cb), cb)], b_all.at[c, mine], once.at[1]
    )
    own_a.start()
    own_b.start()

    barrier = pltpu.get_barrier_semaphore()

    peers = [(i, j) for i in range(n_row) for j in range(n_col) if i or j]
    peers.sort(key=lambda ij: (min(ij) > 0, ij))
    mates = [(i, j) for i, j in peers if min(i, j) == 0]
    for i, j in mates:
        pl.semaphore_signal(barrier, inc=1, device_id=(row_mate(i), col_mate(j)), device_id_type=MESH)
    pl.semaphore_wait(barrier, len(mates))

    def sent(ref, sem):
        remote(ref, ref, sem, sem, (r, c)).wait_send()

    def landed(ref, sem):
        remote(ref, ref, sem, sem, (r, c)).wait_recv()

    def send_a(i):
        dst = row_mate(i)
        cols = pl.ds(pl.multiple_of(dst * rb, rb), rb)
        return remote(a_in.at[:, cols], a_all.at[c, mine], once.at[2], r_a.at[i], (dst, c))

    def got_a(i):
        src = row_mate(n_row - i)
        rows = pl.ds(pl.multiple_of(src * t, t), t)
        return remote(a_all.at[c, rows], a_all.at[c, rows], once.at[2], r_a.at[i], (src, c))

    def send_b(j):
        dst = col_mate(j)
        cols = pl.ds(pl.multiple_of(dst * cb, cb), cb)
        return remote(b_in.at[:, cols], b_all.at[c, mine], once.at[3], r_b.at[z], (r, dst))

    def block(chunk, p):
        return a_all.at[chunk, pl.ds(pl.multiple_of(p * t, t), t)]

    partner = z * 2 + (1 - k)
    above = (r, lax.min(c + 2, n_col - 2 + k))
    below = (r, lax.max(c - 2, k))
    beside = (r, partner)

    def up(chunk, p):
        ref = block(chunk, p)
        return remote(ref, ref, once.at[16], r_line.at[chunk // 2, p], above)

    def down(chunk, p):
        ref = block(chunk, p)
        return remote(ref, ref, once.at[16], r_line.at[chunk // 2 - 1, p], below)

    def across(chunk, p):
        ref = block(chunk, p)
        far = lax.max(chunk // 2 - z, z - chunk // 2) == n_z - 1
        slot = jnp.where(far, n_z + p, chunk // 2)
        return remote(ref, ref, once.at[4], r_across.at[slot], beside)

    widths = [rb >> min(f + 1, TAIL - 1) for f in range(TAIL)]
    slabs = [pl.ds(sum(widths[:f]), widths[f]) for f in range(TAIL)]

    def slab(chunk, p, f):
        return a_all.at[chunk, pl.ds(pl.multiple_of(p * t, t), t), slabs[f]]

    def tail(way, chunk, p, f):
        ref = slab(chunk, p, f)
        return remote(ref, ref, once.at[16], r_tail.at[f], above if way == 0 else below)

    def tail_across(chunk, p, f):
        ref = slab(chunk, p, f)
        return remote(ref, ref, once.at[4], x_tail.at[f], beside)

    can_up = z < n_z - 1
    can_down = z > 0

    def slice_at(o):
        return (r + n_row - o) % n_row

    def send_line(o):
        p = slice_at(o)

        @pl.when(can_up)
        def _():
            up(c, p).start()

        @pl.when(can_down)
        def _():
            down(c, p).start()

        across(c, p).start()

    own_a.wait()
    send_line(0)
    for i in range(1, n_row):
        send_a(i).start()

    for dist in range(n_z - 1, 0, -1):
        for side in range(2):
            zz = z - dist if side == 0 else z + dist

            @pl.when(jnp.logical_and(zz >= 0, zz < n_z))
            def _():
                for other in range(2):
                    send_b((zz * 2 + (k + other) % 2 + n_col - c) % n_col).start()

    send_b((partner + n_col - c) % n_col).start()

    for o in range(1, n_row):
        got_a(o).wait_recv()
        if o < n_row - 1:
            send_line(o)

    def moments_a(q, carry):
        cols = pl.ds(pl.multiple_of(q * 128, 128), 128)
        x = a_all[c, :, cols].astype(F32)
        stat_a[0, 0:1, cols] = jnp.sum(x, 0, keepdims=True)
        stat_a[0, 1:2, cols] = jnp.sum(x * x, 0, keepdims=True)
        return carry

    lax.fori_loop(0, rb // 128, moments_a, 0)

    half = rb // 2
    near = pl.ds(pl.multiple_of(k * half, half), half)
    away = pl.ds(pl.multiple_of((1 - k) * half, half), half)
    give_a = remote(stat_a.at[0, :, away], stat_a.at[1, :, away], once.at[5], once.at[6], beside)
    give_a.start()
    give_a.wait_send()
    landed(stat_a.at[1, :, near], once.at[6])
    sums_a[z] = stat_a[0, :, near] + stat_a[1, :, near]
    for j in range(1, n_z):
        remote(
            sums_a.at[z], sums_a.at[z], once.at[12], once.at[13], (r, (c + 2 * j) % n_col)
        ).start()
    if n_row > 1:
        send_line(n_row - 1)

    def send_fwd(i, g):
        return remote(b_all.at[g, mine], b_all.at[g, mine], once.at[7], r_fwd.at[g // 2], (row_mate(i), c))

    def each_chunk(d, do):
        for side in range(2):
            zz = z - d if side == 0 else z + d
            ok = (zz >= 0) if side == 0 else jnp.logical_and(zz < n_z, d > 0)

            @pl.when(ok)
            def _():
                do(zz * 2 + k, side)
                do(zz * 2 + (1 - k), side)

    def forward(d, carry):
        def do(g, side):
            for i in range(1, n_row):
                send_fwd(i, g).start()

        each_chunk(d, do)
        return carry

    def relay(d, o):
        split = isinstance(d, int) and d == n_z - 2 and o == n_row - 1
        from_low = z - d >= 0
        from_high = z + d < n_z
        low = (z - d) * 2 + k
        high = (z + d) * 2 + k
        p = slice_at(o)

        @pl.when(from_low)
        def _():
            up(low, p).wait_recv()

            @pl.when(can_up)
            def _():
                if split:
                    for f in range(TAIL):
                        tail(0, low, p, f).start()
                else:
                    up(low, p).start()

            across(low, p).start()

        @pl.when(from_high)
        def _():
            down(high, p).wait_recv()

            @pl.when(can_down)
            def _():
                if split:
                    for f in range(TAIL):
                        tail(1, high, p, f).start()
                else:
                    down(high, p).start()

            across(high, p).start()

    def arrive(d):
        for side in range(2):
            zz = z - d if side == 0 else z + d

            @pl.when(jnp.logical_and(zz >= 0, zz < n_z))
            def _():
                landed(b_all.at[pl.ds(zz * 2, 2), mine], r_b.at[zz])

    own_b.wait()
    landed(b_all.at[partner, mine], r_b.at[z])
    forward(0, 0)
    early = n_z > 2
    for o in range(n_row if early else 0):
        relay(1, o)
        if o + 1 < min(n_row, n_z):
            arrive(o + 1)
            forward(o + 1, 0)

    def rest(d, carry):
        arrive(d)
        forward(d, 0)
        return carry

    lax.fori_loop(min(n_row, n_z) if early else 1, n_z, rest, 0)

    for o in range(n_row if n_z > 3 else 0):
        relay(2, o)

    def moments_b(q, carry):
        cols = pl.ds(pl.multiple_of(q * 128, 128), 128)
        total = jnp.zeros((1, 128), F32)
        squares = jnp.zeros((1, 128), F32)
        for g in range(n_col):
            x = b_all[g, mine, cols].astype(F32)
            total = total + jnp.sum(x, 0, keepdims=True)
            squares = squares + jnp.sum(x * x, 0, keepdims=True)
        stat_b[r, 0:1, cols] = total
        stat_b[r, 1:2, cols] = squares
        return carry

    lax.fori_loop(0, cb // 128, moments_b, 0)

    def send_sb(i):
        return remote(stat_b.at[r], stat_b.at[r], once.at[8], once.at[9], (row_mate(i), c))

    for i in range(1, n_row):
        send_sb(i).start()

    def clear(q, carry):
        rows = pl.ds(pl.multiple_of(q * 64, 64), 64)
        out[rows, :] = jnp.zeros((64, cb), F32)
        return carry

    lax.fori_loop(0, rb // 64, clear, 0)

    landed(sums_a.at[pl.ds(0, n_z - 1)], once.at[13])
    total_a[:, near] = jnp.sum(sums_a[...], 0)
    swap_a = remote(total_a.at[:, near], total_a.at[:, near], once.at[14], once.at[15], beside)
    swap_a.start()
    landed(stat_b.at[pl.ds(0, n_row - 1)], once.at[9])

    def coefs(sums, coef):
        mean = sums[0:1] / count
        var = sums[1:2] / count - mean * mean
        coef[0:1, :] = mean
        coef[1:2, :] = lax.rsqrt(var + 1e-05)

    coefs(jnp.sum(stat_b[...], 0), coef_b)
    swap_a.wait_send()
    landed(total_a.at[:, away], once.at[15])
    coefs(total_a[...], coef_a)

    tile = min(1024, rb)

    def wait_fwd(zz):
        landed(b_all.at[pl.ds(zz * 2, 2), pl.ds(0, (n_row - 1) * t)], r_fwd.at[zz])

    def process(zz):
        landed(a_all.at[zz * 2 + (1 - k)], r_across.at[zz])
        wait_fwd(zz)
        multiply(zz, pl.ds(0, n_row * t), n_row * t)

    def normalize_b(zz, rows, height):
        def one(q, carry):
            cols = pl.ds(pl.multiple_of(q * 128, 128), 128)
            x = b_all[pl.ds(zz * 2, 2), rows, cols].astype(F32).reshape(2 * height, 128)
            nb[0 : 2 * height, cols] = ((x - coef_b[0:1, cols]) * coef_b[1:2, cols]).astype(BF16)
            return carry

        lax.fori_loop(0, cb // 128, one, 0)

    def product(zz, rows, height, cols, width):
        x = a_all[pl.ds(zz * 2, 2), rows, cols].astype(F32).reshape(2 * height, width)
        na = ((x - coef_a[0:1, cols]) * coef_a[1:2, cols]).astype(BF16)
        return lax.dot_general(
            na, nb[0 : 2 * height, :], (((0,), (0,)), ((), ())), preferred_element_type=F32
        )

    def multiply(zz, rows, height):
        normalize_b(zz, rows, height)

        def mul(q, carry):
            cols = pl.ds(pl.multiple_of(q * tile, tile), tile)
            out[cols, :] += product(zz, rows, height, cols, tile)
            return carry

        lax.fori_loop(0, rb // tile, mul, 0)

    def process_all(d):
        def one(side, carry):
            zz = jnp.where(side == 0, z - d, z + d)
            ok = jnp.logical_and(zz >= 0, zz < n_z)
            ok = jnp.logical_and(ok, jnp.logical_or(side == 0, d > 0))

            @pl.when(ok)
            def _():
                process(zz)

            return carry

        lax.fori_loop(0, 2, one, 0)

    at_end = jnp.logical_and(n_z > 2, jnp.logical_or(z == 0, z == n_z - 1))

    def finish(x):
        x = x * (1.0 / count)
        partial[...] += jnp.sum((x * x).reshape(x.shape[0] // 8, 8, cb), 0)
        return x

    first = c * cb - r * rb

    def diagonal(start, height):
        @pl.when(jnp.logical_and(first > start - cb, first < start + height))
        def _():
            same = lax.broadcasted_iota(jnp.int32, (128, 128), 0) == lax.broadcasted_iota(
                jnp.int32, (128, 128), 1
            )

            def one(q, carry):
                row = start + q * 128
                col = row - first
                inside = jnp.logical_and(col >= 0, col < cb)
                cols = pl.ds(pl.multiple_of(jnp.where(inside, col, 0), 128), 128)
                x = out[pl.ds(pl.multiple_of(row, 128), 128), cols]
                more = (1.0 - x) * (1.0 - x) - 0.0051 * (x * x)
                more = jnp.where(jnp.logical_and(same, inside), more, 0.0)
                return carry + jnp.sum(more.reshape(16, 8, 128), 0)

            spread[...] += lax.fori_loop(0, height // 128, one, jnp.zeros((8, 128), F32))

    def last():
        zz = jnp.where(z == 0, n_z - 1, 0)
        g = zz * 2 + k
        other = zz * 2 + (1 - k)

        @pl.when(jnp.logical_or(z == 0, z == n_z - 1))
        def _():
            wait_fwd(zz)

            def one(o, carry):
                p = slice_at(o)
                landed(block(g, p), r_line.at[jnp.where(z == 0, n_z - 2, 0), p])
                across(g, p).start()
                landed(block(other, p), r_across.at[n_z + p])
                multiply(zz, pl.ds(pl.multiple_of(p * t, t), t), t)
                return carry

            lax.fori_loop(0, n_row - 1 if n_z > 2 else n_row, one, 0)
            if n_z > 2:
                p = slice_at(n_row - 1)
                rows = pl.ds(pl.multiple_of(p * t, t), t)
                normalize_b(zz, rows, t)

                def take(f):
                    landed(slab(g, p, f), r_tail.at[f])
                    tail_across(g, p, f).start()

                def use(f):
                    landed(slab(other, p, f), x_tail.at[f])
                    cols = slabs[f]
                    out[cols, :] = finish(out[cols, :] + product(zz, rows, t, cols, widths[f]))
                    diagonal(slabs[f].start, widths[f])

                take(0)
                take(1)
                use(0)
                for f in range(2, TAIL):
                    take(f)
                for f in range(1, TAIL):
                    use(f)

    def step(d, carry):
        process_all(d)

        if n_z > 5:
            @pl.when(d + 3 < n_z - 2)
            def _():
                for o in range(n_row):
                    relay(d + 3, o)

        if n_z > 4:
            @pl.when(d + 3 == n_z - 2)
            def _():
                for o in range(n_row):
                    relay(n_z - 2, o)

        return carry

    lax.fori_loop(0, max(n_z - 1, 1), step, 0)
    partial[...] = jnp.zeros((8, cb), F32)
    spread[...] = jnp.zeros((8, 128), F32)
    if n_z > 1:
        last()

    @pl.when(jnp.logical_not(at_end))
    def _():
        def part(q, carry):
            rows = pl.ds(pl.multiple_of(q * 64, 64), 64)
            out[rows, :] = finish(out[rows, :])
            return carry

        lax.fori_loop(0, rb // 64, part, 0)
        diagonal(0, rb)

    folded = partial[:, 0:128]
    for q in range(1, cb // 128):
        folded = folded + partial[:, q * 128 : (q + 1) * 128]
    shares[me] = jnp.sum(0.0051 * folded + spread[...], 0, keepdims=True)

    way = jnp.where(2 * z >= n_z, 1, n_col - 1)
    far_first = sorted(peers, key=lambda ij: (ij[1] == 0, (ij[1] - 2) % n_col, ij[0] % 2 == 0))
    for i, j in far_first:
        to = (row_mate(i), (c + way * j) % n_col)
        remote(shares.at[me], shares.at[me], once.at[10], once.at[11], to).start()

    sent(a_all.at[0, pl.ds(0, (n_row - 1) * t)], once.at[2])
    sent(b_all.at[pl.ds(0, n_col - 1), pl.ds(0, t)], once.at[3])
    sent(sums_a.at[pl.ds(0, n_z - 1)], once.at[12])
    sent(stat_b.at[pl.ds(0, n_row - 1)], once.at[8])
    sent(b_all.at[:, pl.ds(0, (n_row - 1) * t)], once.at[7])
    sent(a_all.at[pl.ds(0, n_z)], once.at[4])

    ends = jnp.logical_or(z == 0, z == n_z - 1)

    @pl.when(ends)
    def _():
        sent(a_all.at[0], once.at[16])

    if n_z > 2:
        @pl.when(jnp.logical_not(ends))
        def _():
            sent(a_all.at[pl.ds(0, n_z + 1)], once.at[16])

    sent(shares.at[pl.ds(0, n_dev - 1)], once.at[10])
    landed(shares.at[pl.ds(0, n_dev - 1)], once.at[11])
    shares_out[...] = shares[...]


def hbm(x):
    return pltpu.with_memory_space_constraint(x, pltpu.HBM)


def emit_body(pieces, width, x, shares, out, loss_out, loss, sem):
    height = x.shape[0] // pieces
    for i in range(pieces):
        rows = pl.ds(i * height, height)
        pltpu.make_async_copy(x.at[rows], out.at[rows], sem.at[0]).start()
    loss[...] = jnp.sum(jnp.sum(shares[...], 0), keepdims=True) / width
    send_loss = pltpu.make_async_copy(loss, loss_out, sem.at[1])
    send_loss.start()
    pltpu.make_async_copy(x, out, sem.at[0]).wait()
    send_loss.wait()


def emit(x, shares, width):
    return pl.pallas_call(
        functools.partial(emit_body, 8, width),
        out_shape=(jax.ShapeDtypeStruct(x.shape, x.dtype), jax.ShapeDtypeStruct((1, 1), F32)),
        in_specs=[pl.BlockSpec(memory_space=pltpu.VMEM)] * 2,
        out_specs=(pl.BlockSpec(memory_space=pltpu.HBM),) * 2,
        scratch_shapes=[pltpu.VMEM((1, 1), F32), pltpu.SemaphoreType.DMA((2,))],
        compiler_params=pltpu.CompilerParams(vmem_limit_bytes=16 << 20),
        name="emit",
    )(x, shares)


def shards(view_a, view_b):
    t, width = view_a.shape
    n_row = lax.axis_size("row")
    n_col = lax.axis_size("col")
    rb = width // n_row
    cb = width // n_col
    count = t * n_row * n_col
    n_chunk = t * n_row
    dma = pltpu.SemaphoreType.DMA
    size = 2 * (count * (rb + cb) + 2 * n_chunk * cb + 2 * t * width) + 4 * rb * cb
    product, shares = pl.pallas_call(
        functools.partial(body, n_row, n_col),
        out_shape=(
            jax.ShapeDtypeStruct((rb, cb), F32),
            jax.ShapeDtypeStruct((n_row * n_col, 1, 128), F32),
        ),
        in_specs=[pl.BlockSpec(memory_space=pltpu.HBM)] * 2,
        out_specs=(pl.BlockSpec(memory_space=pltpu.VMEM),) * 2,
        scratch_shapes=[
            pltpu.VMEM((n_col, n_chunk, rb), BF16),
            pltpu.VMEM((n_col, n_chunk, cb), BF16),
            pltpu.VMEM((2 * n_chunk, cb), BF16),
            pltpu.VMEM((2, 2, rb), F32),
            pltpu.VMEM((n_col // 2, 2, rb // 2), F32),
            pltpu.VMEM((2, rb), F32),
            pltpu.VMEM((n_row, 2, cb), F32),
            pltpu.VMEM((2, rb), F32),
            pltpu.VMEM((2, cb), F32),
            pltpu.VMEM((8, cb), F32),
            pltpu.VMEM((8, 128), F32),
            pltpu.VMEM((n_row * n_col, 1, 128), F32),
            dma((n_row,)), dma((n_col // 2,)),
            dma((max(n_col // 2 - 1, 1), n_row)), dma((n_col // 2 + n_row,)),
            dma((TAIL,)), dma((TAIL,)),
            dma((n_col // 2,)), dma((17,)),
        ],
        compiler_params=pltpu.CompilerParams(
            collective_id=0, has_side_effects=True, vmem_limit_bytes=min(size + (12 << 20), 60 << 20)
        ),
        name="twins",
    )(hbm(view_a), hbm(view_b))
    product, loss = emit(product, shares, width)
    return product, loss.reshape(())


def solution(mesh):
    return jax.shard_map(
        shards,
        mesh=mesh,
        in_specs=(P(("row", "col"), None), P(("row", "col"), None)),
        out_specs=(P("row", "col"), P()),
        check_vma=False,
    )
```

```python
import functools

import jax
import jax.numpy as jnp
from jax import lax
from jax.experimental import pallas as pl
from jax.experimental.pallas import tpu as pltpu
from jax.sharding import PartitionSpec as P

MESH = pl.DeviceIdType.MESH
F32 = jnp.float32
BF16 = jnp.bfloat16


def tail_slabs(rb):
    return min(5, (rb // 128).bit_length())


def body(
    n_row, n_col,
    a_in, b_in, out, shares_out,
    a_all, b_all, nb, stat_a, sums_a, total_a, stat_b, coef_a, coef_b, partial, spread, shares,
    r_a, r_b, r_line, r_across, r_tail, x_tail, r_fwd, once,
):
    t = a_in.shape[0]
    rb = a_in.shape[1] // n_row
    cb = b_in.shape[1] // n_col
    count = t * n_row * n_col
    n_z = n_col // 2
    n_dev = n_row * n_col
    r = lax.axis_index("row")
    c = lax.axis_index("col")
    me = r * n_col + c
    z = c // 2
    k = c % 2
    mine = pl.ds(pl.multiple_of(r * t, t), t)

    def row_mate(i):
        return (r + i) % n_row

    def col_mate(j):
        return (c + j) % n_col

    def remote(src, dst, ss, rs, dev):
        return pltpu.make_async_remote_copy(
            src_ref=src, dst_ref=dst, send_sem=ss, recv_sem=rs, device_id=dev, device_id_type=MESH
        )

    own_a = pltpu.make_async_copy(
        a_in.at[:, pl.ds(pl.multiple_of(r * rb, rb), rb)], a_all.at[c, mine], once.at[0]
    )
    own_b = pltpu.make_async_copy(
        b_in.at[:, pl.ds(pl.multiple_of(c * cb, cb), cb)], b_all.at[c, mine], once.at[1]
    )
    own_a.start()
    own_b.start()

    barrier = pltpu.get_barrier_semaphore()

    peers = [(i, j) for i in range(n_row) for j in range(n_col) if i or j]
    peers.sort(key=lambda ij: (min(ij) > 0, ij))
    mates = [(i, j) for i, j in peers if min(i, j) == 0]
    for i, j in mates:
        pl.semaphore_signal(barrier, inc=1, device_id=(row_mate(i), col_mate(j)), device_id_type=MESH)
    pl.semaphore_wait(barrier, len(mates))

    def sent(ref, sem):
        remote(ref, ref, sem, sem, (r, c)).wait_send()

    def landed(ref, sem):
        remote(ref, ref, sem, sem, (r, c)).wait_recv()

    def send_a(i):
        dst = row_mate(i)
        cols = pl.ds(pl.multiple_of(dst * rb, rb), rb)
        return remote(a_in.at[:, cols], a_all.at[c, mine], once.at[2], r_a.at[i], (dst, c))

    def got_a(i):
        src = row_mate(n_row - i)
        rows = pl.ds(pl.multiple_of(src * t, t), t)
        return remote(a_all.at[c, rows], a_all.at[c, rows], once.at[2], r_a.at[i], (src, c))

    def send_b(j):
        dst = col_mate(j)
        cols = pl.ds(pl.multiple_of(dst * cb, cb), cb)
        return remote(b_in.at[:, cols], b_all.at[c, mine], once.at[3], r_b.at[z], (r, dst))

    def block(chunk, p):
        return a_all.at[chunk, pl.ds(pl.multiple_of(p * t, t), t)]

    partner = z * 2 + (1 - k)
    above = (r, lax.min(c + 2, n_col - 2 + k))
    below = (r, lax.max(c - 2, k))
    beside = (r, partner)

    def up(chunk, p):
        ref = block(chunk, p)
        return remote(ref, ref, once.at[16], r_line.at[chunk // 2, p], above)

    def down(chunk, p):
        ref = block(chunk, p)
        return remote(ref, ref, once.at[16], r_line.at[chunk // 2 - 1, p], below)

    def across(chunk, p):
        ref = block(chunk, p)
        far = lax.max(chunk // 2 - z, z - chunk // 2) == n_z - 1
        slot = jnp.where(far, n_z + p, chunk // 2)
        return remote(ref, ref, once.at[4], r_across.at[slot], beside)

    n_tail = tail_slabs(rb)
    widths = [rb >> min(f + 1, n_tail - 1) for f in range(n_tail)]
    slabs = [pl.ds(sum(widths[:f]), widths[f]) for f in range(n_tail)]

    def slab(chunk, p, f):
        return a_all.at[chunk, pl.ds(pl.multiple_of(p * t, t), t), slabs[f]]

    def tail(way, chunk, p, f):
        ref = slab(chunk, p, f)
        return remote(ref, ref, once.at[16], r_tail.at[f], above if way == 0 else below)

    def tail_across(chunk, p, f):
        ref = slab(chunk, p, f)
        return remote(ref, ref, once.at[4], x_tail.at[f], beside)

    can_up = z < n_z - 1
    can_down = z > 0

    def slice_at(o):
        return (r + n_row - o) % n_row

    def send_line(o):
        p = slice_at(o)

        @pl.when(can_up)
        def _():
            up(c, p).start()

        @pl.when(can_down)
        def _():
            down(c, p).start()

        across(c, p).start()

    own_a.wait()
    send_line(0)
    for i in range(1, n_row):
        send_a(i).start()

    for dist in range(n_z - 1, 0, -1):
        for side in range(2):
            zz = z - dist if side == 0 else z + dist

            @pl.when(jnp.logical_and(zz >= 0, zz < n_z))
            def _():
                for other in range(2):
                    send_b((zz * 2 + (k + other) % 2 + n_col - c) % n_col).start()

    send_b((partner + n_col - c) % n_col).start()

    for o in range(1, n_row):
        got_a(o).wait_recv()
        if o < n_row - 1:
            send_line(o)

    def moments_a(q, carry):
        cols = pl.ds(pl.multiple_of(q * 128, 128), 128)
        x = a_all[c, :, cols].astype(F32)
        stat_a[0, 0:1, cols] = jnp.sum(x, 0, keepdims=True)
        stat_a[0, 1:2, cols] = jnp.sum(x * x, 0, keepdims=True)
        return carry

    lax.fori_loop(0, rb // 128, moments_a, 0)

    half = rb // 2
    near = pl.ds(pl.multiple_of(k * half, half), half)
    away = pl.ds(pl.multiple_of((1 - k) * half, half), half)
    give_a = remote(stat_a.at[0, :, away], stat_a.at[1, :, away], once.at[5], once.at[6], beside)
    give_a.start()
    give_a.wait_send()
    landed(stat_a.at[1, :, near], once.at[6])
    sums_a[z] = stat_a[0, :, near] + stat_a[1, :, near]
    for j in range(1, n_z):
        remote(
            sums_a.at[z], sums_a.at[z], once.at[12], once.at[13], (r, (c + 2 * j) % n_col)
        ).start()
    if n_row > 1:
        send_line(n_row - 1)

    def send_fwd(i, g):
        return remote(b_all.at[g, mine], b_all.at[g, mine], once.at[7], r_fwd.at[g // 2], (row_mate(i), c))

    def each_chunk(d, do):
        for side in range(2):
            zz = z - d if side == 0 else z + d
            ok = (zz >= 0) if side == 0 else jnp.logical_and(zz < n_z, d > 0)

            @pl.when(ok)
            def _():
                do(zz * 2 + k, side)
                do(zz * 2 + (1 - k), side)

    def forward(d, carry):
        def do(g, side):
            for i in range(1, n_row):
                send_fwd(i, g).start()

        each_chunk(d, do)
        return carry

    def relay(d, o):
        split = isinstance(d, int) and d == n_z - 2 and o == n_row - 1
        from_low = z - d >= 0
        from_high = z + d < n_z
        low = (z - d) * 2 + k
        high = (z + d) * 2 + k
        p = slice_at(o)

        @pl.when(from_low)
        def _():
            up(low, p).wait_recv()

            @pl.when(can_up)
            def _():
                if split:
                    for f in range(n_tail):
                        tail(0, low, p, f).start()
                else:
                    up(low, p).start()

            across(low, p).start()

        @pl.when(from_high)
        def _():
            down(high, p).wait_recv()

            @pl.when(can_down)
            def _():
                if split:
                    for f in range(n_tail):
                        tail(1, high, p, f).start()
                else:
                    down(high, p).start()

            across(high, p).start()

    def arrive(d):
        for side in range(2):
            zz = z - d if side == 0 else z + d

            @pl.when(jnp.logical_and(zz >= 0, zz < n_z))
            def _():
                landed(b_all.at[pl.ds(zz * 2, 2), mine], r_b.at[zz])

    own_b.wait()
    landed(b_all.at[partner, mine], r_b.at[z])
    forward(0, 0)
    early = n_z > 2
    for o in range(n_row if early else 0):
        relay(1, o)
        if o + 1 < min(n_row, n_z):
            arrive(o + 1)
            forward(o + 1, 0)

    def rest(d, carry):
        arrive(d)
        forward(d, 0)
        return carry

    lax.fori_loop(min(n_row, n_z) if early else 1, n_z, rest, 0)

    for o in range(n_row if n_z > 3 else 0):
        relay(2, o)

    def moments_b(q, carry):
        cols = pl.ds(pl.multiple_of(q * 128, 128), 128)
        total = jnp.zeros((1, 128), F32)
        squares = jnp.zeros((1, 128), F32)
        for g in range(n_col):
            x = b_all[g, mine, cols].astype(F32)
            total = total + jnp.sum(x, 0, keepdims=True)
            squares = squares + jnp.sum(x * x, 0, keepdims=True)
        stat_b[r, 0:1, cols] = total
        stat_b[r, 1:2, cols] = squares
        return carry

    lax.fori_loop(0, cb // 128, moments_b, 0)

    def send_sb(i):
        return remote(stat_b.at[r], stat_b.at[r], once.at[8], once.at[9], (row_mate(i), c))

    for i in range(1, n_row):
        send_sb(i).start()

    def clear(q, carry):
        rows = pl.ds(pl.multiple_of(q * 64, 64), 64)
        out[rows, :] = jnp.zeros((64, cb), F32)
        return carry

    lax.fori_loop(0, rb // 64, clear, 0)

    landed(sums_a.at[pl.ds(0, n_z - 1)], once.at[13])
    total_a[:, near] = jnp.sum(sums_a[...], 0)
    swap_a = remote(total_a.at[:, near], total_a.at[:, near], once.at[14], once.at[15], beside)
    swap_a.start()
    landed(stat_b.at[pl.ds(0, n_row - 1)], once.at[9])

    def coefs(sums, coef):
        mean = sums[0:1] / count
        var = sums[1:2] / count - mean * mean
        coef[0:1, :] = mean
        coef[1:2, :] = lax.rsqrt(var + 1e-05)

    coefs(jnp.sum(stat_b[...], 0), coef_b)
    swap_a.wait_send()
    landed(total_a.at[:, away], once.at[15])
    coefs(total_a[...], coef_a)

    tile = min(1024, rb)

    def wait_fwd(zz):
        landed(b_all.at[pl.ds(zz * 2, 2), pl.ds(0, (n_row - 1) * t)], r_fwd.at[zz])

    def process(zz):
        landed(a_all.at[zz * 2 + (1 - k)], r_across.at[zz])
        wait_fwd(zz)
        multiply(zz, pl.ds(0, n_row * t), n_row * t)

    def normalize_b(zz, rows, height):
        def one(q, carry):
            cols = pl.ds(pl.multiple_of(q * 128, 128), 128)
            x = b_all[pl.ds(zz * 2, 2), rows, cols].astype(F32).reshape(2 * height, 128)
            nb[0 : 2 * height, cols] = ((x - coef_b[0:1, cols]) * coef_b[1:2, cols]).astype(BF16)
            return carry

        lax.fori_loop(0, cb // 128, one, 0)

    def product(zz, rows, height, cols, width):
        x = a_all[pl.ds(zz * 2, 2), rows, cols].astype(F32).reshape(2 * height, width)
        na = ((x - coef_a[0:1, cols]) * coef_a[1:2, cols]).astype(BF16)
        return lax.dot_general(
            na, nb[0 : 2 * height, :], (((0,), (0,)), ((), ())), preferred_element_type=F32
        )

    def multiply(zz, rows, height):
        normalize_b(zz, rows, height)

        def mul(q, carry):
            cols = pl.ds(pl.multiple_of(q * tile, tile), tile)
            out[cols, :] += product(zz, rows, height, cols, tile)
            return carry

        lax.fori_loop(0, rb // tile, mul, 0)

    def process_all(d):
        def one(side, carry):
            zz = jnp.where(side == 0, z - d, z + d)
            ok = jnp.logical_and(zz >= 0, zz < n_z)
            ok = jnp.logical_and(ok, jnp.logical_or(side == 0, d > 0))

            @pl.when(ok)
            def _():
                process(zz)

            return carry

        lax.fori_loop(0, 2, one, 0)

    at_end = jnp.logical_and(n_z > 2, jnp.logical_or(z == 0, z == n_z - 1))

    def finish(x):
        x = x * (1.0 / count)
        partial[...] += jnp.sum((x * x).reshape(x.shape[0] // 8, 8, cb), 0)
        return x

    first = c * cb - r * rb

    def diagonal(start, height):
        @pl.when(jnp.logical_and(first > start - cb, first < start + height))
        def _():
            same = lax.broadcasted_iota(jnp.int32, (128, 128), 0) == lax.broadcasted_iota(
                jnp.int32, (128, 128), 1
            )

            def one(q, carry):
                row = start + q * 128
                col = row - first
                inside = jnp.logical_and(col >= 0, col < cb)
                cols = pl.ds(pl.multiple_of(jnp.where(inside, col, 0), 128), 128)
                x = out[pl.ds(pl.multiple_of(row, 128), 128), cols]
                more = (1.0 - x) * (1.0 - x) - 0.0051 * (x * x)
                more = jnp.where(jnp.logical_and(same, inside), more, 0.0)
                return carry + jnp.sum(more.reshape(16, 8, 128), 0)

            spread[...] += lax.fori_loop(0, height // 128, one, jnp.zeros((8, 128), F32))

    def last():
        zz = jnp.where(z == 0, n_z - 1, 0)
        g = zz * 2 + k
        other = zz * 2 + (1 - k)

        @pl.when(jnp.logical_or(z == 0, z == n_z - 1))
        def _():
            wait_fwd(zz)

            def one(o, carry):
                p = slice_at(o)
                landed(block(g, p), r_line.at[jnp.where(z == 0, n_z - 2, 0), p])
                across(g, p).start()
                landed(block(other, p), r_across.at[n_z + p])
                multiply(zz, pl.ds(pl.multiple_of(p * t, t), t), t)
                return carry

            lax.fori_loop(0, n_row - 1 if n_z > 2 else n_row, one, 0)
            if n_z > 2:
                p = slice_at(n_row - 1)
                rows = pl.ds(pl.multiple_of(p * t, t), t)
                normalize_b(zz, rows, t)

                def take(f):
                    landed(slab(g, p, f), r_tail.at[f])
                    tail_across(g, p, f).start()

                def use(f):
                    landed(slab(other, p, f), x_tail.at[f])
                    cols = slabs[f]
                    out[cols, :] = finish(out[cols, :] + product(zz, rows, t, cols, widths[f]))
                    diagonal(slabs[f].start, widths[f])

                take(0)
                for f in range(1, n_tail):
                    take(f)
                    use(f - 1)
                use(n_tail - 1)

    def step(d, carry):
        process_all(d)

        if n_z > 5:
            @pl.when(d + 3 < n_z - 2)
            def _():
                for o in range(n_row):
                    relay(d + 3, o)

        if n_z > 4:
            @pl.when(d + 3 == n_z - 2)
            def _():
                for o in range(n_row):
                    relay(n_z - 2, o)

        return carry

    lax.fori_loop(0, max(n_z - 1, 1), step, 0)
    partial[...] = jnp.zeros((8, cb), F32)
    spread[...] = jnp.zeros((8, 128), F32)
    if n_z > 1:
        last()

    @pl.when(jnp.logical_not(at_end))
    def _():
        def part(q, carry):
            rows = pl.ds(pl.multiple_of(q * 64, 64), 64)
            out[rows, :] = finish(out[rows, :])
            return carry

        lax.fori_loop(0, rb // 64, part, 0)
        diagonal(0, rb)

    folded = partial[:, 0:128]
    for q in range(1, cb // 128):
        folded = folded + partial[:, q * 128 : (q + 1) * 128]
    shares[me] = jnp.sum(0.0051 * folded + spread[...], 0, keepdims=True)

    way = jnp.where(2 * z >= n_z, 1, n_col - 1)
    far_first = sorted(peers, key=lambda ij: (ij[1] == 0, (ij[1] - 2) % n_col, ij[0] % 2 == 0))
    for i, j in far_first:
        to = (row_mate(i), (c + way * j) % n_col)
        remote(shares.at[me], shares.at[me], once.at[10], once.at[11], to).start()

    sent(a_all.at[0, pl.ds(0, (n_row - 1) * t)], once.at[2])
    sent(b_all.at[pl.ds(0, n_col - 1), pl.ds(0, t)], once.at[3])
    sent(sums_a.at[pl.ds(0, n_z - 1)], once.at[12])
    sent(stat_b.at[pl.ds(0, n_row - 1)], once.at[8])
    sent(b_all.at[:, pl.ds(0, (n_row - 1) * t)], once.at[7])
    sent(a_all.at[pl.ds(0, n_z)], once.at[4])

    ends = jnp.logical_or(z == 0, z == n_z - 1)

    @pl.when(ends)
    def _():
        sent(a_all.at[0], once.at[16])

    if n_z > 2:
        @pl.when(jnp.logical_not(ends))
        def _():
            sent(a_all.at[pl.ds(0, n_z + 1)], once.at[16])

    sent(shares.at[pl.ds(0, n_dev - 1)], once.at[10])
    landed(shares.at[pl.ds(0, n_dev - 1)], once.at[11])
    shares_out[...] = shares[...]


def hbm(x):
    return pltpu.with_memory_space_constraint(x, pltpu.HBM)


def emit_body(pieces, width, x, shares, out, loss_out, loss, sem):
    height = x.shape[0] // pieces
    for i in range(pieces):
        rows = pl.ds(i * height, height)
        pltpu.make_async_copy(x.at[rows], out.at[rows], sem.at[0]).start()
    loss[...] = jnp.sum(jnp.sum(shares[...], 0), keepdims=True) / width
    send_loss = pltpu.make_async_copy(loss, loss_out, sem.at[1])
    send_loss.start()
    pltpu.make_async_copy(x, out, sem.at[0]).wait()
    send_loss.wait()


def emit(x, shares, width):
    return pl.pallas_call(
        functools.partial(emit_body, 8, width),
        out_shape=(jax.ShapeDtypeStruct(x.shape, x.dtype), jax.ShapeDtypeStruct((1, 1), F32)),
        in_specs=[pl.BlockSpec(memory_space=pltpu.VMEM)] * 2,
        out_specs=(pl.BlockSpec(memory_space=pltpu.HBM),) * 2,
        scratch_shapes=[pltpu.VMEM((1, 1), F32), pltpu.SemaphoreType.DMA((2,))],
        compiler_params=pltpu.CompilerParams(vmem_limit_bytes=16 << 20),
        name="emit",
    )(x, shares)


def shards(view_a, view_b):
    t, width = view_a.shape
    n_row = lax.axis_size("row")
    n_col = lax.axis_size("col")
    rb = width // n_row
    cb = width // n_col
    count = t * n_row * n_col
    n_chunk = t * n_row
    dma = pltpu.SemaphoreType.DMA
    size = 2 * (count * (rb + cb) + 2 * n_chunk * cb + 2 * t * width) + 4 * rb * cb
    product, shares = pl.pallas_call(
        functools.partial(body, n_row, n_col),
        out_shape=(
            jax.ShapeDtypeStruct((rb, cb), F32),
            jax.ShapeDtypeStruct((n_row * n_col, 1, 128), F32),
        ),
        in_specs=[pl.BlockSpec(memory_space=pltpu.HBM)] * 2,
        out_specs=(pl.BlockSpec(memory_space=pltpu.VMEM),) * 2,
        scratch_shapes=[
            pltpu.VMEM((n_col, n_chunk, rb), BF16),
            pltpu.VMEM((n_col, n_chunk, cb), BF16),
            pltpu.VMEM((2 * n_chunk, cb), BF16),
            pltpu.VMEM((2, 2, rb), F32),
            pltpu.VMEM((n_col // 2, 2, rb // 2), F32),
            pltpu.VMEM((2, rb), F32),
            pltpu.VMEM((n_row, 2, cb), F32),
            pltpu.VMEM((2, rb), F32),
            pltpu.VMEM((2, cb), F32),
            pltpu.VMEM((8, cb), F32),
            pltpu.VMEM((8, 128), F32),
            pltpu.VMEM((n_row * n_col, 1, 128), F32),
            dma((n_row,)), dma((n_col // 2,)),
            dma((max(n_col // 2 - 1, 1), n_row)), dma((n_col // 2 + n_row,)),
            dma((tail_slabs(rb),)), dma((tail_slabs(rb),)),
            dma((n_col // 2,)), dma((17,)),
        ],
        compiler_params=pltpu.CompilerParams(
            collective_id=0, has_side_effects=True, vmem_limit_bytes=min(size + (12 << 20), 60 << 20)
        ),
        name="twins",
    )(hbm(view_a), hbm(view_b))
    product, loss = emit(product, shares, width)
    return product, loss.reshape(())


def solution(mesh):
    return jax.shard_map(
        shards,
        mesh=mesh,
        in_specs=(P(("row", "col"), None), P(("row", "col"), None)),
        out_specs=(P("row", "col"), P()),
        check_vma=False,
    )
```
